8 devices in a mesh: rep: 1 (over z), sub: 2 (over y), blk: 4 (over x, core).
Axes of the slice: x: 2, y: 2, z: 1, core: 2. Of those that a mesh axis runs over, the one named last changes fastest.
Arguments:
- ratings: float32 [8192, 4096], P(('rep', 'blk', 'sub'))
- mask: int32 [8192, 4096], P(('rep', 'blk', 'sub'))
- user_init: float32 [8192, 96], P(('rep', 'blk', 'sub'))
- item_init: float32 [4096, 96], P(('rep', 'blk'))
Outputs:
- output 1: float32 [8192, 96], P(('rep', 'blk', 'sub'))
- output 2: float32 [4096, 96], P(('rep', 'blk'))
All inputs are finite; a program needn't handle non-finite values.
Results may differ from the reference program's by a relative error of at most 0.001.
Values are sent between devices in bfloat16 or wider.
A program may use at most 1 GiB of HBM per device.

```python
import math
import jax
import jax.numpy as jnp
from jax import lax

BLOCKS = 4
SUB_SHARDS = 2
USERS_DEV = 1024
ITEMS_DEV = 1024
RANK = 96
STEPS = 4
EPOCHS = 2

USERS_BLK = SUB_SHARDS * USERS_DEV
USERS = BLOCKS * USERS_BLK
ITEMS = BLOCKS * ITEMS_DEV
BIG_SIDE = max(ITEMS_DEV, USERS_BLK)
STEP_SIZE = 0.4 * math.sqrt(RANK) / (math.sqrt(BIG_SIDE) + math.sqrt(RANK)) ** 2
WEIGHT_DECAY = 0.002 / STEP_SIZE


def setup_inputs(seed: int = 0, part: int = 0) -> dict:
    part_key = jax.random.fold_in(jax.random.key(seed), part)
    keys = jax.random.split(part_key, 7)
    user_true = jax.random.normal(keys[0], (USERS, RANK), jnp.float32)
    item_true = jax.random.normal(keys[1], (ITEMS, RANK), jnp.float32)
    noise = jax.random.normal(keys[2], (USERS, ITEMS), jnp.float32)
    ratings = jnp.dot(user_true, item_true.T) / math.sqrt(RANK) + 0.3 * noise
    block_pct = jax.random.randint(keys[3], (BLOCKS, 1, BLOCKS, 1), 10, 51)
    draws = jax.random.randint(keys[4], (BLOCKS, USERS_BLK, BLOCKS, ITEMS_DEV), 0, 100)
    mask = (draws < block_pct).astype(jnp.int32).reshape(USERS, ITEMS)
    init_scale = RANK ** -0.25
    user_init = jax.random.normal(keys[5], (USERS, RANK), jnp.float32) * init_scale
    item_init = jax.random.normal(keys[6], (ITEMS, RANK), jnp.float32) * init_scale
    return {'ratings': ratings, 'mask': mask, 'user_init': user_init, 'item_init': item_init}


def reference(ratings, mask, user_init, item_init):
    rating_blk = ratings.reshape(BLOCKS, USERS_BLK, BLOCKS, ITEMS_DEV)
    mask_blk = mask.reshape(BLOCKS, USERS_BLK, BLOCKS, ITEMS_DEV).astype(jnp.float32)
    block_ids = jnp.arange(BLOCKS)

    def sub_epoch(state, offset):
        cols = (block_ids + offset) % BLOCKS
        rating_now = rating_blk[block_ids, :, cols, :]
        mask_now = mask_blk[block_ids, :, cols, :]

        def grad_step(inner, unused):
            users, items = inner
            user_half = users.astype(jnp.bfloat16).astype(jnp.float32)
            item_half = items.astype(jnp.bfloat16).astype(jnp.float32)
            predicted = jnp.einsum('bur,bir->bui', user_half, item_half)
            err_half = (mask_now * (predicted - rating_now)).astype(jnp.bfloat16).astype(jnp.float32)
            grad_user = jnp.einsum('bui,bir->bur', err_half, item_half) + WEIGHT_DECAY * users
            grad_item = jnp.einsum('bui,bur->bir', err_half, user_half) + WEIGHT_DECAY * items
            return (users - STEP_SIZE * grad_user, items - STEP_SIZE * grad_item), None

        inner, unused = lax.scan(grad_step, state, None, length=STEPS)
        return (inner[0], jnp.roll(inner[1], -1, axis=0)), None

    start = (user_init.reshape(BLOCKS, USERS_BLK, RANK), item_init.reshape(BLOCKS, ITEMS_DEV, RANK))
    offsets = jnp.tile(block_ids, EPOCHS)
    final, unused = lax.scan(sub_epoch, start, offsets)
    return final[0].reshape(USERS, RANK), final[1].reshape(ITEMS, RANK)
```

```python
import functools
import math

import jax
import jax.numpy as jnp
from jax import lax
from jax.experimental import pallas as pl
from jax.experimental.pallas import tpu as pltpu
from jax.sharding import PartitionSpec as P

STEPS = 4
EPOCHS = 2
STEP_GAIN = 0.4
DECAY = 0.002
CHUNK = 128
ROWS = 256
MESH = pl.DeviceIdType.MESH
NT = (((1,), (1,)), ((), ()))


def run(n_blk, eta, lam, r_hbm, m_hbm, u_hbm, v_hbm, u_out, v_out,
        rate, known, err, users, users_bf, users_t, own, own_bf, own_next, part, send_p, recv_p,
        peer_v, in_v, last_v, v_start, edge_f, edge_b,
        load_sem, uv_sem, p_send, p_recv, v_send, v_recv,
        ef_send, ef_recv, eb_send, eb_recv, el_send, el_recv):
    rank, n_users = users.shape
    half = own.shape[1]
    n_chunks = half // CHUNK
    n_sub_epochs = EPOCHS * n_blk
    pad = users_bf.shape[1] - rank
    me = lax.axis_index('sub')
    other = 1 - me
    blk = lax.axis_index('blk')
    down = lax.rem(blk + n_blk - 1, n_blk)
    up = lax.rem(blk + 1, n_blk)

    def load(t, role):
        owner = me if role else other
        col = pl.multiple_of(lax.rem(blk + t, n_blk) * (2 * half) + owner * half, half)
        return [
            pltpu.make_async_copy(src.at[:, pl.ds(col, half)], dst.at[t, role], load_sem.at[t, role, j])
            for j, (src, dst) in enumerate(((r_hbm, rate), (m_hbm, known)))
        ]

    def start_load(t):
        for role in range(2):
            for copy in load(t, role):
                copy.start()

    u_copy = pltpu.make_async_copy(u_hbm, users, uv_sem.at[0])
    v_copy = pltpu.make_async_copy(v_hbm, v_start, uv_sem.at[1])
    u_copy.start()
    v_copy.start()
    start_load(0)

    barrier = pltpu.get_barrier_semaphore()
    friends = [(blk, other), (down, me), (down, other), (up, me), (up, other)]
    for b, s in friends:
        pl.semaphore_signal(barrier, inc=1, device_id={'sub': s, 'blk': b}, device_id_type=MESH)

    def refresh_users(u):
        u_bf = u.astype(jnp.bfloat16)
        users_t[...] = u_bf
        wide = jnp.concatenate([u, jnp.zeros((pad, n_users), jnp.float32)], axis=0)
        users_bf[...] = wide.T.astype(jnp.bfloat16)

    u_copy.wait()
    refresh_users(users[...])
    v_copy.wait()
    for c in range(n_chunks):
        mine = pl.ds(pl.multiple_of(me * half + c * CHUNK, CHUNK), CHUNK)
        theirs = pl.ds(pl.multiple_of(other * half + c * CHUNK, CHUNK), CHUNK)
        in_v[0, c] = v_start[:, mine]
        peer_v[0, c] = v_start[:, theirs].astype(jnp.bfloat16)
    pl.semaphore_wait(barrier, len(friends))

    def remote(src, dst, send, recv, s, b):
        return pltpu.make_async_remote_copy(
            src_ref=src, dst_ref=dst, send_sem=send, recv_sem=recv,
            device_id={'sub': s, 'blk': b}, device_id_type=MESH)

    def part_copy(k, slot, c):
        return remote(send_p.at[slot, c], recv_p.at[k, c], p_send.at[slot, c], p_recv.at[slot, c], other, blk)

    def item_copy(k, q, c):
        return remote(own_next.at[q, c], peer_v.at[k + 1, c], v_send.at[q, c], v_recv.at[c], other, blk)

    def edge_own(t, c):
        slot = lax.rem(t, 2)
        return remote(edge_f.at[slot, c], in_v.at[t + 1, c], ef_send.at[slot, c], ef_recv.at[t, c], me, down)

    def edge_peer(t, c):
        slot = lax.rem(t, 2)
        return remote(edge_b.at[slot, c], peer_v.at[STEPS * (t + 1), c], eb_send.at[slot, c], eb_recv.at[t, c], other, down)

    def edge_last(t, c):
        slot = lax.rem(t, 2)
        return remote(edge_f.at[slot, c], last_v.at[c], el_send.at[c], el_recv.at[c], other, down)

    def widen(v):
        return jnp.concatenate([v, jnp.zeros((pad, v.shape[1]), v.dtype)], axis=0)

    def errors(tm, role, cols, v_bf):
        v_wide = widen(v_bf)
        for r in range(0, n_users, ROWS):
            rows = pl.ds(r, ROWS)
            pred = jnp.dot(users_bf[rows, :], v_wide, preferred_element_type=jnp.float32)
            diff = jnp.where(known[tm, role, rows, cols] != 0, pred - rate[tm, role, rows, cols], 0.0)
            err[role, rows, cols] = diff.astype(jnp.bfloat16)

    def sub_epoch(t, carry):
        tm = lax.rem(t, n_blk)
        for q in range(STEPS):
            k = STEPS * t + q
            slot = q % 2
            if q == 0:
                @pl.when(t < n_blk)
                def _():
                    for copy in load(t, 0):
                        copy.wait()
            for c in range(n_chunks):
                if q == 0:
                    @pl.when(t > 0)
                    def _():
                        edge_peer(t - 1, c).wait_recv()
                else:
                    item_copy(k - 1, q - 1, c).wait_recv()
                cols = pl.ds(c * CHUNK, CHUNK)
                errors(tm, 0, cols, peer_v[k, c])
                total = jnp.dot(users_t[...], err[0, :, cols], preferred_element_type=jnp.float32)
                if q < 2:
                    @pl.when(t > 0)
                    def _():
                        part_copy(k - 2, slot, c).wait_send()
                else:
                    part_copy(k - 2, slot, c).wait_send()
                send_p[slot, c] = total
                part_copy(k, slot, c).start()
            if q == 0:
                @pl.when(t + 1 < n_blk)
                def _():
                    start_load(t + 1)

                @pl.when(t < n_blk)
                def _():
                    for copy in load(t, 1):
                        copy.wait()
                for c in range(n_chunks):
                    @pl.when(t > 0)
                    def _():
                        edge_own(t - 1, c).wait_recv()
                    v = in_v[t, c]
                    own[:, pl.ds(c * CHUNK, CHUNK)] = v
                    own_bf[:, pl.ds(c * CHUNK, CHUNK)] = v.astype(jnp.bfloat16)
            for c in range(0, half, 256):
                cols = pl.ds(c, 256)
                errors(tm, 1, cols, own_bf[:, cols])
                part[:, cols] = jnp.dot(users_t[...], err[1, :, cols], preferred_element_type=jnp.float32)
            v_peer = jnp.concatenate([peer_v[k, c] for c in range(n_chunks)], axis=1)
            v_own = own_bf[...]
            for r in range(0, n_users, ROWS):
                rows = pl.ds(r, ROWS)
                grad = lax.dot_general(v_peer, err[0, rows, :], NT, preferred_element_type=jnp.float32)
                grad += lax.dot_general(v_own, err[1, rows, :], NT, preferred_element_type=jnp.float32)
                u = users[:, rows]
                users[:, rows] = u - eta * (grad + lam * u)
            refresh_users(users[...])
            for c in range(n_chunks):
                cols = pl.ds(c * CHUNK, CHUNK)
                part_copy(k, slot, c).wait_recv()
                v = own[:, cols]
                v = v - eta * ((part[:, cols] + recv_p[k, c]) + lam * v)
                if q < STEPS - 1:
                    own[:, cols] = v
                    v_bf = v.astype(jnp.bfloat16)
                    own_bf[:, cols] = v_bf

                    @pl.when(t > 0)
                    def _():
                        item_copy(k - STEPS, q, c).wait_send()
                    own_next[q, c] = v_bf
                    item_copy(k, q, c).start()
                else:
                    @pl.when(t > 1)
                    def _():
                        edge_own(t - 2, c).wait_send()
                        edge_peer(t - 2, c).wait_send()
                    edge_slot = lax.rem(t, 2)
                    edge_f[edge_slot, c] = v
                    edge_b[edge_slot, c] = v.astype(jnp.bfloat16)

                    @pl.when(t < n_sub_epochs - 1)
                    def _():
                        edge_peer(t, c).start()

                    @pl.when(t == n_sub_epochs - 1)
                    def _():
                        edge_last(t, c).start()
                    edge_own(t, c).start()
        return carry

    lax.fori_loop(0, n_sub_epochs, sub_epoch, 0)

    u_back = pltpu.make_async_copy(users, u_out, uv_sem.at[0])
    u_back.start()
    end = n_sub_epochs - 1
    last_k = STEPS * n_sub_epochs - 1
    for c in range(n_chunks):
        mine = pl.ds(pl.multiple_of(me * half + c * CHUNK, CHUNK), CHUNK)
        theirs = pl.ds(pl.multiple_of(other * half + c * CHUNK, CHUNK), CHUNK)
        edge_own(end, c).wait_recv()
        v_start[:, mine] = in_v[n_sub_epochs, c]
        edge_last(end, c).wait_recv()
        v_start[:, theirs] = last_v[c]
    v_back = pltpu.make_async_copy(v_start, v_out, uv_sem.at[1])
    v_back.start()
    for c in range(n_chunks):
        part_copy(last_k - 1, 0, c).wait_send()
        part_copy(last_k, 1, c).wait_send()
        for q in range(STEPS - 1):
            item_copy(STEPS * end + q, q, c).wait_send()
        edge_own(end - 1, c).wait_send()
        edge_peer(end - 1, c).wait_send()
        edge_own(end, c).wait_send()
        edge_last(end, c).wait_send()
    u_back.wait()
    v_back.wait()


def solution(mesh):
    n_blk = mesh.shape['blk']
    n_sub = mesh.shape['sub']
    row_spec = P(('rep', 'blk', 'sub'), None)
    item_spec = P(('rep', 'blk'), None)

    def local_run(ratings, mask, user_init, item_init):
        n_users = ratings.shape[0]
        n_items, rank = item_init.shape
        half = n_items // n_sub
        n_chunks = half // CHUNK
        n_sub_epochs = EPOCHS * n_blk
        n_steps = STEPS * n_sub_epochs
        wide = 128
        big_side = max(n_items, n_sub * n_users)
        eta = STEP_GAIN * math.sqrt(rank) / (math.sqrt(big_side) + math.sqrt(rank)) ** 2
        lam = DECAY / eta
        f32, bf16 = jnp.float32, jnp.bfloat16
        dma = pltpu.SemaphoreType.DMA
        chunk = (rank, CHUNK)
        any_space = pl.BlockSpec(memory_space=pl.ANY)
        users_t, items_t = pl.pallas_call(
            functools.partial(run, n_blk, eta, lam),
            out_shape=[jax.ShapeDtypeStruct((rank, n_users), f32), jax.ShapeDtypeStruct((rank, n_items), f32)],
            in_specs=[any_space] * 4,
            out_specs=[any_space] * 2,
            scratch_shapes=[
                pltpu.VMEM((n_blk, 2, n_users, half), f32),
                pltpu.VMEM((n_blk, 2, n_users, half), jnp.int32),
                pltpu.VMEM((2, n_users, half), bf16),
                pltpu.VMEM((rank, n_users), f32),
                pltpu.VMEM((n_users, wide), bf16),
                pltpu.VMEM((rank, n_users), bf16),
                pltpu.VMEM((rank, half), f32),
                pltpu.VMEM((rank, half), bf16),
                pltpu.VMEM((STEPS - 1, n_chunks) + chunk, bf16),
                pltpu.VMEM((rank, half), f32),
                pltpu.VMEM((2, n_chunks) + chunk, f32),
                pltpu.VMEM((n_steps, n_chunks) + chunk, f32),
                pltpu.VMEM((n_steps + 1, n_chunks) + chunk, bf16),
                pltpu.VMEM((n_sub_epochs + 1, n_chunks) + chunk, f32),
                pltpu.VMEM((n_chunks,) + chunk, f32),
                pltpu.VMEM((rank, n_items), f32),
                pltpu.VMEM((2, n_chunks) + chunk, f32),
                pltpu.VMEM((2, n_chunks) + chunk, bf16),
                dma((n_blk, 2, 2)),
                dma((2,)),
                dma((2, n_chunks)),
                dma((2, n_chunks)),
                dma((STEPS - 1, n_chunks)),
                dma((n_chunks,)),
                dma((2, n_chunks)),
                dma((n_sub_epochs, n_chunks)),
                dma((2, n_chunks)),
                dma((n_sub_epochs, n_chunks)),
                dma((n_chunks,)),
                dma((n_chunks,)),
            ],
            compiler_params=pltpu.CompilerParams(
                collective_id=0, has_side_effects=True, vmem_limit_bytes=64_000_000),
        )(ratings, mask, user_init.T, item_init.T)
        return users_t.T, items_t.T

    return jax.shard_map(local_run, mesh=mesh, in_specs=(row_spec, row_spec, row_spec, item_spec), out_specs=(row_spec, item_spec), check_vma=False)
```

```python
import functools
import math

import jax
import jax.numpy as jnp
from jax import lax
from jax.experimental import pallas as pl
from jax.experimental.pallas import tpu as pltpu
from jax.sharding import PartitionSpec as P

STEPS = 4
EPOCHS = 2
STEP_GAIN = 0.4
DECAY = 0.002
CHUNK = 128
ROWS = 256
PIECES = 2
MESH = pl.DeviceIdType.MESH
NT = (((1,), (1,)), ((), ()))


def run(n_blk, eta, lam, r_hbm, m_hbm, u_hbm, v_hbm, u_out, v_out,
        rate, known, err, users, users_bf, users_t, own, own_bf, own_next, part, send_p, recv_p,
        peer_v, in_v, last_v, v_start, edge_f, edge_b,
        load_sem, uv_sem, p_send, p_recv, v_send, v_recv,
        ef_send, ef_recv, eb_send, eb_recv, el_send, el_recv):
    rank, n_users = users.shape
    half = own.shape[1]
    n_chunks = half // CHUNK
    n_sub_epochs = EPOCHS * n_blk
    pad = users_bf.shape[1] - rank
    me = lax.axis_index('sub')
    other = 1 - me
    blk = lax.axis_index('blk')
    down = lax.rem(blk + n_blk - 1, n_blk)
    up = lax.rem(blk + 1, n_blk)

    def load(t, role):
        owner = me if role else other
        col = pl.multiple_of(lax.rem(blk + t, n_blk) * (2 * half) + owner * half, half)
        return [
            pltpu.make_async_copy(src.at[:, pl.ds(col, half)], dst.at[t, role], load_sem.at[t, role, j])
            for j, (src, dst) in enumerate(((r_hbm, rate), (m_hbm, known)))
        ]

    def start_load(t):
        for role in range(2):
            for copy in load(t, role):
                copy.start()

    u_copy = pltpu.make_async_copy(u_hbm, users, uv_sem.at[0])
    v_copy = pltpu.make_async_copy(v_hbm, v_start, uv_sem.at[1])
    u_copy.start()
    v_copy.start()
    start_load(0)

    barrier = pltpu.get_barrier_semaphore()
    friends = [(blk, other), (down, me), (down, other), (up, me), (up, other)]
    for b, s in friends:
        pl.semaphore_signal(barrier, inc=1, device_id={'sub': s, 'blk': b}, device_id_type=MESH)

    def refresh_users(u):
        u_bf = u.astype(jnp.bfloat16)
        users_t[...] = u_bf
        wide = jnp.concatenate([u, jnp.zeros((pad, n_users), jnp.float32)], axis=0)
        users_bf[...] = wide.T.astype(jnp.bfloat16)

    u_copy.wait()
    refresh_users(users[...])
    v_copy.wait()
    for c in range(n_chunks):
        mine = pl.ds(pl.multiple_of(me * half + c * CHUNK, CHUNK), CHUNK)
        theirs = pl.ds(pl.multiple_of(other * half + c * CHUNK, CHUNK), CHUNK)
        in_v[0, c] = v_start[:, mine]
        peer_v[0, c] = v_start[:, theirs].astype(jnp.bfloat16)
    pl.semaphore_wait(barrier, len(friends))

    def remote(src, dst, send, recv, s, b):
        return pltpu.make_async_remote_copy(
            src_ref=src, dst_ref=dst, send_sem=send, recv_sem=recv,
            device_id={'sub': s, 'blk': b}, device_id_type=MESH)

    piece = rank // PIECES

    def part_copy(k, slot, c, p):
        at = pl.ds(p * piece, piece)
        return remote(send_p.at[slot, c, at], recv_p.at[k, c, at], p_send.at[slot, c, p], p_recv.at[slot, c, p], other, blk)

    def item_copy(k, q, c, p):
        at = pl.ds(p * piece, piece)
        return remote(own_next.at[q, c, at], peer_v.at[k + 1, c, at], v_send.at[q, c, p], v_recv.at[c, p], other, blk)

    def edge_own(t, c):
        slot = lax.rem(t, 2)
        return remote(edge_f.at[slot, c], in_v.at[t + 1, c], ef_send.at[slot, c], ef_recv.at[t, c], me, down)

    def edge_peer(t, c):
        slot = lax.rem(t, 2)
        return remote(edge_b.at[slot, c], peer_v.at[STEPS * (t + 1), c], eb_send.at[slot, c], eb_recv.at[t, c], other, down)

    def edge_last(t, c):
        slot = lax.rem(t, 2)
        return remote(edge_f.at[slot, c], last_v.at[c], el_send.at[c], el_recv.at[c], other, down)

    def widen(v):
        return jnp.concatenate([v, jnp.zeros((pad, v.shape[1]), v.dtype)], axis=0)

    def errors(tm, role, cols, v_bf):
        v_wide = widen(v_bf)
        for r in range(0, n_users, ROWS):
            rows = pl.ds(r, ROWS)
            pred = jnp.dot(users_bf[rows, :], v_wide, preferred_element_type=jnp.float32)
            diff = jnp.where(known[tm, role, rows, cols] != 0, pred - rate[tm, role, rows, cols], 0.0)
            err[role, rows, cols] = diff.astype(jnp.bfloat16)

    def sub_epoch(t, carry):
        tm = lax.rem(t, n_blk)
        for q in range(STEPS):
            k = STEPS * t + q
            slot = q % 2
            if q == 0:
                @pl.when(t < n_blk)
                def _():
                    for copy in load(t, 0):
                        copy.wait()
            for c in range(n_chunks):
                if q == 0:
                    @pl.when(t > 0)
                    def _():
                        edge_peer(t - 1, c).wait_recv()
                else:
                    for p in range(PIECES):
                        item_copy(k - 1, q - 1, c, p).wait_recv()
                cols = pl.ds(c * CHUNK, CHUNK)
                errors(tm, 0, cols, peer_v[k, c])
                total = jnp.dot(users_t[...], err[0, :, cols], preferred_element_type=jnp.float32)
                for p in range(PIECES):
                    if q < 2:
                        @pl.when(t > 0)
                        def _():
                            part_copy(k - 2, slot, c, p).wait_send()
                    else:
                        part_copy(k - 2, slot, c, p).wait_send()
                send_p[slot, c] = total
                for p in range(PIECES):
                    part_copy(k, slot, c, p).start()
            if q == 0:
                @pl.when(t + 1 < n_blk)
                def _():
                    start_load(t + 1)

                @pl.when(t < n_blk)
                def _():
                    for copy in load(t, 1):
                        copy.wait()
                for c in range(n_chunks):
                    @pl.when(t > 0)
                    def _():
                        edge_own(t - 1, c).wait_recv()
                    v = in_v[t, c]
                    own[:, pl.ds(c * CHUNK, CHUNK)] = v
                    own_bf[:, pl.ds(c * CHUNK, CHUNK)] = v.astype(jnp.bfloat16)
            for c in range(0, half, 256):
                cols = pl.ds(c, 256)
                errors(tm, 1, cols, own_bf[:, cols])
                part[:, cols] = jnp.dot(users_t[...], err[1, :, cols], preferred_element_type=jnp.float32)
            v_peer = jnp.concatenate([peer_v[k, c] for c in range(n_chunks)], axis=1)
            v_own = own_bf[...]
            for r in range(0, n_users, ROWS):
                rows = pl.ds(r, ROWS)
                grad = lax.dot_general(v_peer, err[0, rows, :], NT, preferred_element_type=jnp.float32)
                grad += lax.dot_general(v_own, err[1, rows, :], NT, preferred_element_type=jnp.float32)
                u = users[:, rows]
                users[:, rows] = u - eta * (grad + lam * u)
            refresh_users(users[...])
            for c in range(n_chunks):
                cols = pl.ds(c * CHUNK, CHUNK)
                if q < STEPS - 1:
                    @pl.when(t > 0)
                    def _():
                        for p in range(PIECES):
                            item_copy(k - STEPS, q, c, p).wait_send()
                else:
                    @pl.when(t > 1)
                    def _():
                        edge_own(t - 2, c).wait_send()
                        edge_peer(t - 2, c).wait_send()
                for p in range(PIECES):
                    at = pl.ds(p * piece, piece)
                    part_copy(k, slot, c, p).wait_recv()
                    v = own[at, cols]
                    v = v - eta * ((part[at, cols] + recv_p[k, c, at]) + lam * v)
                    v_bf = v.astype(jnp.bfloat16)
                    if q < STEPS - 1:
                        own_next[q, c, at] = v_bf
                        item_copy(k, q, c, p).start()
                        own[at, cols] = v
                        own_bf[at, cols] = v_bf
                    else:
                        edge_slot = lax.rem(t, 2)
                        edge_f[edge_slot, c, at] = v
                        edge_b[edge_slot, c, at] = v_bf
                if q == STEPS - 1:
                    @pl.when(t < n_sub_epochs - 1)
                    def _():
                        edge_peer(t, c).start()

                    @pl.when(t == n_sub_epochs - 1)
                    def _():
                        edge_last(t, c).start()
                    edge_own(t, c).start()
        return carry

    lax.fori_loop(0, n_sub_epochs, sub_epoch, 0)

    u_back = pltpu.make_async_copy(users, u_out, uv_sem.at[0])
    u_back.start()
    end = n_sub_epochs - 1
    last_k = STEPS * n_sub_epochs - 1
    for c in range(n_chunks):
        mine = pl.ds(pl.multiple_of(me * half + c * CHUNK, CHUNK), CHUNK)
        theirs = pl.ds(pl.multiple_of(other * half + c * CHUNK, CHUNK), CHUNK)
        edge_own(end, c).wait_recv()
        v_start[:, mine] = in_v[n_sub_epochs, c]
        edge_last(end, c).wait_recv()
        v_start[:, theirs] = last_v[c]
    v_back = pltpu.make_async_copy(v_start, v_out, uv_sem.at[1])
    v_back.start()
    for c in range(n_chunks):
        for p in range(PIECES):
            part_copy(last_k - 1, 0, c, p).wait_send()
            part_copy(last_k, 1, c, p).wait_send()
            for q in range(STEPS - 1):
                item_copy(STEPS * end + q, q, c, p).wait_send()
        edge_own(end - 1, c).wait_send()
        edge_peer(end - 1, c).wait_send()
        edge_own(end, c).wait_send()
        edge_last(end, c).wait_send()
    u_back.wait()
    v_back.wait()


def solution(mesh):
    n_blk = mesh.shape['blk']
    n_sub = mesh.shape['sub']
    row_spec = P(('rep', 'blk', 'sub'), None)
    item_spec = P(('rep', 'blk'), None)

    def local_run(ratings, mask, user_init, item_init):
        n_users = ratings.shape[0]
        n_items, rank = item_init.shape
        half = n_items // n_sub
        n_chunks = half // CHUNK
        n_sub_epochs = EPOCHS * n_blk
        n_steps = STEPS * n_sub_epochs
        wide = 128
        big_side = max(n_items, n_sub * n_users)
        eta = STEP_GAIN * math.sqrt(rank) / (math.sqrt(big_side) + math.sqrt(rank)) ** 2
        lam = DECAY / eta
        f32, bf16 = jnp.float32, jnp.bfloat16
        dma = pltpu.SemaphoreType.DMA
        chunk = (rank, CHUNK)
        any_space = pl.BlockSpec(memory_space=pl.ANY)
        users_t, items_t = pl.pallas_call(
            functools.partial(run, n_blk, eta, lam),
            out_shape=[jax.ShapeDtypeStruct((rank, n_users), f32), jax.ShapeDtypeStruct((rank, n_items), f32)],
            in_specs=[any_space] * 4,
            out_specs=[any_space] * 2,
            scratch_shapes=[
                pltpu.VMEM((n_blk, 2, n_users, half), f32),
                pltpu.VMEM((n_blk, 2, n_users, half), jnp.int32),
                pltpu.VMEM((2, n_users, half), bf16),
                pltpu.VMEM((rank, n_users), f32),
                pltpu.VMEM((n_users, wide), bf16),
                pltpu.VMEM((rank, n_users), bf16),
                pltpu.VMEM((rank, half), f32),
                pltpu.VMEM((rank, half), bf16),
                pltpu.VMEM((STEPS - 1, n_chunks) + chunk, bf16),
                pltpu.VMEM((rank, half), f32),
                pltpu.VMEM((2, n_chunks) + chunk, f32),
                pltpu.VMEM((n_steps, n_chunks) + chunk, f32),
                pltpu.VMEM((n_steps + 1, n_chunks) + chunk, bf16),
                pltpu.VMEM((n_sub_epochs + 1, n_chunks) + chunk, f32),
                pltpu.VMEM((n_chunks,) + chunk, f32),
                pltpu.VMEM((rank, n_items), f32),
                pltpu.VMEM((2, n_chunks) + chunk, f32),
                pltpu.VMEM((2, n_chunks) + chunk, bf16),
                dma((n_blk, 2, 2)),
                dma((2,)),
                dma((2, n_chunks, PIECES)),
                dma((2, n_chunks, PIECES)),
                dma((STEPS - 1, n_chunks, PIECES)),
                dma((n_chunks, PIECES)),
                dma((2, n_chunks)),
                dma((n_sub_epochs, n_chunks)),
                dma((2, n_chunks)),
                dma((n_sub_epochs, n_chunks)),
                dma((n_chunks,)),
                dma((n_chunks,)),
            ],
            compiler_params=pltpu.CompilerParams(
                collective_id=0, has_side_effects=True, vmem_limit_bytes=64_000_000),
        )(ratings, mask, user_init.T, item_init.T)
        return users_t.T, items_t.T

    return jax.shard_map(local_run, mesh=mesh, in_specs=(row_spec, row_spec, row_spec, item_spec), out_specs=(row_spec, item_spec), check_vma=False)
```

```python
import functools
import math

import jax
import jax.numpy as jnp
from jax import lax
from jax.experimental import pallas as pl
from jax.experimental.pallas import tpu as pltpu
from jax.sharding import PartitionSpec as P

STEPS = 4
EPOCHS = 2
STEP_GAIN = 0.4
DECAY = 0.002
CHUNK = 128
ROWS = 256
PIECES = 2
ORDERS = (
    ('A0', 'A1', 'A2', 'A3', 'B', 'C0', 'M', 'C1', 'C2', 'C3'),
    ('A0', 'A1', 'D2', 'D3', 'B', 'C0', 'A2', 'C1', 'A3', 'M'),
)
MESH = pl.DeviceIdType.MESH
NT = (((1,), (1,)), ((), ()))


def run(n_blk, eta, lam, r_hbm, m_hbm, u_hbm, v_hbm, u_out, v_out,
        rate, known, err, users, users_bf, users_t, own, own_bf, own_next, part, send_p, recv_p,
        peer_v, in_v, v_start, edge_f, edge_b,
        load_sem, uv_sem, p_send, p_recv, v_send, v_recv,
        ef_send, ef_recv, eb_send, eb_recv, el_send, el_recv):
    rank, n_users = users.shape
    half = own.shape[1]
    n_chunks = half // CHUNK
    n_sub_epochs = EPOCHS * n_blk
    pad = users_bf.shape[1] - rank
    me = lax.axis_index('sub')
    other = 1 - me
    blk = lax.axis_index('blk')
    down = lax.rem(blk + n_blk - 1, n_blk)
    up = lax.rem(blk + 1, n_blk)

    def load(t, role):
        owner = me if role else other
        col = pl.multiple_of(lax.rem(blk + t, n_blk) * (2 * half) + owner * half, half)
        return [
            pltpu.make_async_copy(src.at[:, pl.ds(col, half)], dst.at[t, role], load_sem.at[t, role, j])
            for j, (src, dst) in enumerate(((r_hbm, rate), (m_hbm, known)))
        ]

    def start_load(t):
        for role in range(2):
            for copy in load(t, role):
                copy.start()

    u_copy = pltpu.make_async_copy(u_hbm, users, uv_sem.at[0])
    v_copy = pltpu.make_async_copy(v_hbm, v_start, uv_sem.at[1])
    u_copy.start()
    v_copy.start()
    for copy in load(0, 0):
        copy.start()

    barrier = pltpu.get_barrier_semaphore()
    friends = [(blk, other), (down, me), (down, other), (up, me), (up, other)]
    for b, s in friends:
        pl.semaphore_signal(barrier, inc=1, device_id={'sub': s, 'blk': b}, device_id_type=MESH)

    def refresh_users(u):
        u_bf = u.astype(jnp.bfloat16)
        users_t[...] = u_bf
        wide = jnp.concatenate([u, jnp.zeros((pad, n_users), jnp.float32)], axis=0)
        users_bf[...] = wide.T.astype(jnp.bfloat16)

    u_copy.wait()
    refresh_users(users[...])
    v_copy.wait()

    def mine(c):
        return pl.ds(pl.multiple_of(me * half + c * CHUNK, CHUNK), CHUNK)

    for c in range(n_chunks):
        theirs = pl.ds(pl.multiple_of(other * half + c * CHUNK, CHUNK), CHUNK)
        in_v[0, c] = v_start[:, mine(c)]
        peer_v[0, c] = v_start[:, theirs].astype(jnp.bfloat16)
    for copy in load(0, 0):
        copy.wait()
    for copy in load(0, 1):
        copy.start()
    pl.semaphore_wait(barrier, len(friends))

    def remote(src, dst, send, recv, s, b):
        return pltpu.make_async_remote_copy(
            src_ref=src, dst_ref=dst, send_sem=send, recv_sem=recv,
            device_id={'sub': s, 'blk': b}, device_id_type=MESH)

    piece = rank // PIECES

    def part_copy(k, slot, c, p):
        at = pl.ds(p * piece, piece)
        return remote(send_p.at[slot, c, at], recv_p.at[k, c, at], p_send.at[slot, c, p], p_recv.at[slot, c, p], other, blk)

    def item_copy(k, q, c, p):
        at = pl.ds(p * piece, piece)
        return remote(own_next.at[q, c, at], peer_v.at[k + 1, c, at], v_send.at[q, c, p], v_recv.at[c, p], other, blk)

    def edge_own(t, c):
        slot = lax.rem(t, 2)
        return remote(edge_f.at[slot, c], in_v.at[t + 1, c], ef_send.at[slot, c], ef_recv.at[t, c], me, down)

    def edge_peer(t, c):
        slot = lax.rem(t, 2)
        return remote(edge_b.at[slot, c], peer_v.at[STEPS * (t + 1), c], eb_send.at[slot, c], eb_recv.at[t, c], other, down)

    def edge_last(t, c):
        slot = lax.rem(t, 2)
        return remote(edge_f.at[slot, c], v_out.at[:, mine(c)], el_send.at[c], el_recv.at[c], other, down)

    def edge_end(t, c):
        slot = lax.rem(t, 2)
        return remote(edge_f.at[slot, c], v_out.at[:, mine(c)], ef_send.at[slot, c], ef_recv.at[t, c], me, down)

    def widen(v):
        return jnp.concatenate([v, jnp.zeros((pad, v.shape[1]), v.dtype)], axis=0)

    def errors(tm, role, cols, v_bf):
        v_wide = widen(v_bf)
        for r in range(0, n_users, ROWS):
            rows = pl.ds(r, ROWS)
            pred = jnp.dot(users_bf[rows, :], v_wide, preferred_element_type=jnp.float32)
            diff = jnp.where(known[tm, role, rows, cols] != 0, pred - rate[tm, role, rows, cols], 0.0)
            err[role, rows, cols] = diff.astype(jnp.bfloat16)

    def send_part(t, q, c):
        k, slot = STEPS * t + q, q % 2
        if q == 0:
            @pl.when(t > 0)
            def _():
                edge_peer(t - 1, c).wait_recv()
        else:
            for p in range(PIECES):
                item_copy(k - 1, q - 1, c, p).wait_recv()
        cols = pl.ds(c * CHUNK, CHUNK)
        errors(lax.rem(t, n_blk), 0, cols, peer_v[k, c])
        total = jnp.dot(users_t[...], err[0, :, cols], preferred_element_type=jnp.float32)
        for p in range(PIECES):
            if q < 2:
                @pl.when(t > 0)
                def _():
                    part_copy(k - 2, slot, c, p).wait_send()
            else:
                part_copy(k - 2, slot, c, p).wait_send()
        send_p[slot, c] = total
        for p in range(PIECES):
            part_copy(k, slot, c, p).start()

    def own_part(t, q):
        if q == 0:
            @pl.when(t + 1 < n_blk)
            def _():
                start_load(t + 1)

            @pl.when(t < n_blk)
            def _():
                for copy in load(t, 1):
                    copy.wait()
            for c in range(n_chunks):
                @pl.when(t > 0)
                def _():
                    edge_own(t - 1, c).wait_recv()
                v = in_v[t, c]
                own[:, pl.ds(c * CHUNK, CHUNK)] = v
                own_bf[0, :, pl.ds(c * CHUNK, CHUNK)] = v.astype(jnp.bfloat16)
        for c in range(0, half, 256):
            cols = pl.ds(c, 256)
            errors(lax.rem(t, n_blk), 1, cols, own_bf[q % 2, :, cols])
            part[:, cols] = jnp.dot(users_t[...], err[1, :, cols], preferred_element_type=jnp.float32)

    def step_users(t, q):
        k = STEPS * t + q
        v_peer = jnp.concatenate([peer_v[k, c] for c in range(n_chunks)], axis=1)
        v_own = own_bf[q % 2]
        for r in range(0, n_users, ROWS):
            rows = pl.ds(r, ROWS)
            grad = lax.dot_general(v_peer, err[0, rows, :], NT, preferred_element_type=jnp.float32)
            grad += lax.dot_general(v_own, err[1, rows, :], NT, preferred_element_type=jnp.float32)
            u = users[:, rows]
            users[:, rows] = u - eta * (grad + lam * u)
        refresh_users(users[...])

    def step_items(t, q, c):
        k, slot = STEPS * t + q, q % 2
        cols = pl.ds(c * CHUNK, CHUNK)
        edge_slot = lax.rem(t, 2)
        if q < STEPS - 1:
            @pl.when(t > 0)
            def _():
                for p in range(PIECES):
                    item_copy(k - STEPS, q, c, p).wait_send()
        else:
            @pl.when(t > 1)
            def _():
                edge_own(t - 2, c).wait_send()
                edge_peer(t - 2, c).wait_send()
        for p in range(PIECES):
            at = pl.ds(p * piece, piece)
            part_copy(k, slot, c, p).wait_recv()
            v = own[at, cols]
            v = v - eta * ((part[at, cols] + recv_p[k, c, at]) + lam * v)
            v_bf = v.astype(jnp.bfloat16)
            if q < STEPS - 1:
                own_next[q, c, at] = v_bf
                item_copy(k, q, c, p).start()
                own[at, cols] = v
                own_bf[(q + 1) % 2, at, cols] = v_bf
            else:
                edge_f[edge_slot, c, at] = v
                edge_b[edge_slot, c, at] = v_bf
        if q == STEPS - 1:
            @pl.when(t < n_sub_epochs - 1)
            def _():
                edge_peer(t, c).start()
                edge_own(t, c).start()

            @pl.when(t == n_sub_epochs - 1)
            def _():
                edge_last(t, c).start()
                edge_end(t, c).start()

    def sub_epoch(t, carry):
        @pl.when((t > 0) & (t < n_blk))
        def _():
            for copy in load(t, 0):
                copy.wait()
        for core, order in enumerate(ORDERS):
            @pl.when(lax.rem(blk, 2) == core)
            def _():
                for q in range(STEPS):
                    for op in order:
                        c = int(op[1:] or 0)
                        if op[0] == 'A':
                            send_part(t, q, c)
                        elif op[0] == 'D' and q > 0:
                            step_items(t, q - 1, c)
                        elif op[0] == 'B':
                            own_part(t, q)
                        elif op[0] == 'C':
                            step_items(t, q, c)
                        elif op[0] == 'M':
                            step_users(t, q)
                for op in order:
                    if op[0] == 'D':
                        step_items(t, STEPS - 1, int(op[1:]))
        return carry

    lax.fori_loop(0, n_sub_epochs, sub_epoch, 0)

    u_back = pltpu.make_async_copy(users, u_out, uv_sem.at[0])
    u_back.start()
    end = n_sub_epochs - 1
    last_k = STEPS * n_sub_epochs - 1
    for c in range(n_chunks):
        edge_end(end, c).wait_recv()
        edge_last(end, c).wait_recv()
    for c in range(n_chunks):
        for p in range(PIECES):
            part_copy(last_k - 1, 0, c, p).wait_send()
            part_copy(last_k, 1, c, p).wait_send()
            for q in range(STEPS - 1):
                item_copy(STEPS * end + q, q, c, p).wait_send()
        edge_own(end - 1, c).wait_send()
        edge_peer(end - 1, c).wait_send()
        edge_end(end, c).wait_send()
        edge_last(end, c).wait_send()
    u_back.wait()


def solution(mesh):
    n_blk = mesh.shape['blk']
    n_sub = mesh.shape['sub']
    row_spec = P(('rep', 'blk', 'sub'), None)
    item_spec = P(('rep', 'blk'), None)

    def local_run(ratings, mask, user_init, item_init):
        n_users = ratings.shape[0]
        n_items, rank = item_init.shape
        half = n_items // n_sub
        n_chunks = half // CHUNK
        n_sub_epochs = EPOCHS * n_blk
        n_steps = STEPS * n_sub_epochs
        wide = 128
        big_side = max(n_items, n_sub * n_users)
        eta = STEP_GAIN * math.sqrt(rank) / (math.sqrt(big_side) + math.sqrt(rank)) ** 2
        lam = DECAY / eta
        f32, bf16 = jnp.float32, jnp.bfloat16
        dma = pltpu.SemaphoreType.DMA
        chunk = (rank, CHUNK)
        any_space = pl.BlockSpec(memory_space=pl.ANY)
        users_t, items_t = pl.pallas_call(
            functools.partial(run, n_blk, eta, lam),
            out_shape=[jax.ShapeDtypeStruct((rank, n_users), f32), jax.ShapeDtypeStruct((rank, n_items), f32)],
            in_specs=[any_space] * 4,
            out_specs=[any_space] * 2,
            scratch_shapes=[
                pltpu.VMEM((n_blk, 2, n_users, half), f32),
                pltpu.VMEM((n_blk, 2, n_users, half), jnp.int32),
                pltpu.VMEM((2, n_users, half), bf16),
                pltpu.VMEM((rank, n_users), f32),
                pltpu.VMEM((n_users, wide), bf16),
                pltpu.VMEM((rank, n_users), bf16),
                pltpu.VMEM((rank, half), f32),
                pltpu.VMEM((2, rank, half), bf16),
                pltpu.VMEM((STEPS - 1, n_chunks) + chunk, bf16),
                pltpu.VMEM((rank, half), f32),
                pltpu.VMEM((2, n_chunks) + chunk, f32),
                pltpu.VMEM((n_steps, n_chunks) + chunk, f32),
                pltpu.VMEM((n_steps + 1, n_chunks) + chunk, bf16),
                pltpu.VMEM((n_sub_epochs, n_chunks) + chunk, f32),
                pltpu.VMEM((rank, n_items), f32),
                pltpu.VMEM((2, n_chunks) + chunk, f32),
                pltpu.VMEM((2, n_chunks) + chunk, bf16),
                dma((n_blk, 2, 2)),
                dma((2,)),
                dma((2, n_chunks, PIECES)),
                dma((2, n_chunks, PIECES)),
                dma((STEPS - 1, n_chunks, PIECES)),
                dma((n_chunks, PIECES)),
                dma((2, n_chunks)),
                dma((n_sub_epochs, n_chunks)),
                dma((2, n_chunks)),
                dma((n_sub_epochs, n_chunks)),
                dma((n_chunks,)),
                dma((n_chunks,)),
            ],
            compiler_params=pltpu.CompilerParams(
                collective_id=0, has_side_effects=True, vmem_limit_bytes=64_000_000),
        )(ratings, mask, user_init.T, item_init.T)
        return users_t.T, items_t.T

    return jax.shard_map(local_run, mesh=mesh, in_specs=(row_spec, row_spec, row_spec, item_spec), out_specs=(row_spec, item_spec), check_vma=False)
```

```python
import functools
import math

import jax
import jax.numpy as jnp
from jax import lax
from jax.experimental import pallas as pl
from jax.experimental.pallas import tpu as pltpu
from jax.sharding import PartitionSpec as P

STEPS = 4
EPOCHS = 2
STEP_GAIN = 0.4
DECAY = 0.002
CHUNK = 128
ROWS = 256
PIECES = 2
ORDERS = (
    ('A0', 'A1', 'A2', 'A3', 'B', 'C0', 'M', 'C1', 'C2', 'C3'),
    ('A0', 'A1', 'D2', 'D3', 'B', 'C0', 'A2', 'C1', 'A3', 'M'),
)
MESH = pl.DeviceIdType.MESH
NT = (((1,), (1,)), ((), ()))


def run(n_blk, eta, lam, r_hbm, m_hbm, u_hbm, v_hbm, u_out, v_out,
        rate, known, err, users, users_bf, users_t, own, own_bf, own_next, part, send_p, recv_p,
        peer_v, in_v, v_start, edge_f, edge_b,
        load_sem, uv_sem, p_send, p_recv, v_send, v_recv,
        ef_send, ef_recv, eb_send, eb_recv, el_send, el_recv):
    rank, n_users = users.shape
    half = own.shape[1]
    n_chunks = half // CHUNK
    n_sub_epochs = EPOCHS * n_blk
    pad = users_bf.shape[1] - rank
    me = lax.axis_index('sub')
    other = 1 - me
    blk = lax.axis_index('blk')
    down = lax.rem(blk + n_blk - 1, n_blk)
    up = lax.rem(blk + 1, n_blk)

    def load(t, role):
        owner = me if role else other
        col = pl.multiple_of(lax.rem(blk + t, n_blk) * (2 * half) + owner * half, half)
        return [
            pltpu.make_async_copy(src.at[:, pl.ds(col, half)], dst.at[t, role], load_sem.at[t, role, j])
            for j, (src, dst) in enumerate(((r_hbm, rate), (m_hbm, known)))
        ]

    def start_load(t):
        for role in range(2):
            for copy in load(t, role):
                copy.start()

    u_copy = pltpu.make_async_copy(u_hbm, users, uv_sem.at[0])
    v_copy = pltpu.make_async_copy(v_hbm, v_start, uv_sem.at[1])
    u_copy.start()
    v_copy.start()
    for copy in load(0, 0):
        copy.start()

    barrier = pltpu.get_barrier_semaphore()
    friends = [(blk, other), (down, me), (down, other), (up, me), (up, other)]
    for b, s in friends:
        pl.semaphore_signal(barrier, inc=1, device_id={'sub': s, 'blk': b}, device_id_type=MESH)

    def refresh_users(u):
        u_bf = u.astype(jnp.bfloat16)
        users_t[...] = u_bf
        wide = jnp.concatenate([u, jnp.zeros((pad, n_users), jnp.float32)], axis=0)
        users_bf[...] = wide.T.astype(jnp.bfloat16)

    u_copy.wait()
    refresh_users(users[...])
    v_copy.wait()

    def mine(c):
        return pl.ds(pl.multiple_of(me * half + c * CHUNK, CHUNK), CHUNK)

    for c in range(n_chunks):
        theirs = pl.ds(pl.multiple_of(other * half + c * CHUNK, CHUNK), CHUNK)
        in_v[0, c] = v_start[:, mine(c)]
        peer_v[0, c] = v_start[:, theirs].astype(jnp.bfloat16)
    for copy in load(0, 0):
        copy.wait()
    for copy in load(0, 1):
        copy.start()
    pl.semaphore_wait(barrier, len(friends))

    def remote(src, dst, send, recv, s, b):
        return pltpu.make_async_remote_copy(
            src_ref=src, dst_ref=dst, send_sem=send, recv_sem=recv,
            device_id={'sub': s, 'blk': b}, device_id_type=MESH)

    piece = rank // PIECES

    def part_copy(k, slot, c, p):
        at = pl.ds(p * piece, piece)
        return remote(send_p.at[slot, c, at], recv_p.at[k, c, at], p_send.at[slot, c, p], p_recv.at[slot, c, p], other, blk)

    def item_copy(k, q, c, p):
        at = pl.ds(p * piece, piece)
        return remote(own_next.at[q, c, at], peer_v.at[k + 1, c, at], v_send.at[q, c, p], v_recv.at[c, p], other, blk)

    def edge_own(t, c):
        slot = lax.rem(t, 2)
        return remote(edge_f.at[slot, c], in_v.at[t + 1, c], ef_send.at[slot, c], ef_recv.at[t, c], me, down)

    def edge_peer(t, c):
        slot = lax.rem(t, 2)
        return remote(edge_b.at[slot, c], peer_v.at[STEPS * (t + 1), c], eb_send.at[slot, c], eb_recv.at[t, c], other, down)

    def edge_last(t, c):
        slot = lax.rem(t, 2)
        return remote(edge_f.at[slot, c], v_out.at[:, mine(c)], el_send.at[c], el_recv.at[c], other, down)

    def edge_end(t, c):
        slot = lax.rem(t, 2)
        return remote(edge_f.at[slot, c], v_out.at[:, mine(c)], ef_send.at[slot, c], ef_recv.at[t, c], me, down)

    def widen(v):
        return jnp.concatenate([v, jnp.zeros((pad, v.shape[1]), v.dtype)], axis=0)

    def errors(tm, role, cols, v_bf):
        v_wide = widen(v_bf)
        for r in range(0, n_users, ROWS):
            rows = pl.ds(r, ROWS)
            pred = jnp.dot(users_bf[rows, :], v_wide, preferred_element_type=jnp.float32)
            diff = jnp.where(known[tm, role, rows, cols] != 0, pred - rate[tm, role, rows, cols], 0.0)
            err[role, rows, cols] = diff.astype(jnp.bfloat16)

    def send_part(t, q, c):
        k, slot = STEPS * t + q, q % 2
        if q == 0:
            @pl.when(t > 0)
            def _():
                edge_peer(t - 1, c).wait_recv()
        else:
            for p in range(PIECES):
                item_copy(k - 1, q - 1, c, p).wait_recv()
        cols = pl.ds(c * CHUNK, CHUNK)
        errors(lax.rem(t, n_blk), 0, cols, peer_v[k, c])
        total = jnp.dot(users_t[...], err[0, :, cols], preferred_element_type=jnp.float32)
        for p in range(PIECES):
            if q < 2:
                @pl.when(t > 0)
                def _():
                    part_copy(k - 2, slot, c, p).wait_send()
            else:
                part_copy(k - 2, slot, c, p).wait_send()
        send_p[slot, c] = total
        for p in range(PIECES):
            part_copy(k, slot, c, p).start()

    def own_part(t, q):
        if q == 0:
            @pl.when(t + 1 < n_blk)
            def _():
                start_load(t + 1)

            @pl.when(t < n_blk)
            def _():
                for copy in load(t, 1):
                    copy.wait()
            for c in range(n_chunks):
                @pl.when(t > 0)
                def _():
                    edge_own(t - 1, c).wait_recv()
                v = in_v[t, c]
                own[:, pl.ds(c * CHUNK, CHUNK)] = v
                own_bf[0, :, pl.ds(c * CHUNK, CHUNK)] = v.astype(jnp.bfloat16)
        for c in range(0, half, 256):
            cols = pl.ds(c, 256)
            errors(lax.rem(t, n_blk), 1, cols, own_bf[q % 2, :, cols])
            part[:, cols] = jnp.dot(users_t[...], err[1, :, cols], preferred_element_type=jnp.float32)

    def step_users(t, q):
        k = STEPS * t + q
        v_peer = jnp.concatenate([peer_v[k, c] for c in range(n_chunks)], axis=1)
        v_own = own_bf[q % 2]
        for r in range(0, n_users, ROWS):
            rows = pl.ds(r, ROWS)
            grad = lax.dot_general(v_peer, err[0, rows, :], NT, preferred_element_type=jnp.float32)
            grad += lax.dot_general(v_own, err[1, rows, :], NT, preferred_element_type=jnp.float32)
            u = users[:, rows]
            users[:, rows] = u - eta * (grad + lam * u)
        refresh_users(users[...])

    def step_items(t, q, c):
        k, slot = STEPS * t + q, q % 2
        cols = pl.ds(c * CHUNK, CHUNK)
        edge_slot = lax.rem(t, 2)
        if q < STEPS - 1:
            @pl.when(t > 0)
            def _():
                for p in range(PIECES):
                    item_copy(k - STEPS, q, c, p).wait_send()
        else:
            @pl.when(t > 1)
            def _():
                edge_own(t - 2, c).wait_send()
                edge_peer(t - 2, c).wait_send()
        for p in range(PIECES):
            at = pl.ds(p * piece, piece)
            part_copy(k, slot, c, p).wait_recv()
            v = own[at, cols]
            v = v - eta * ((part[at, cols] + recv_p[k, c, at]) + lam * v)
            v_bf = v.astype(jnp.bfloat16)
            if q < STEPS - 1:
                own_next[q, c, at] = v_bf
                item_copy(k, q, c, p).start()
                own[at, cols] = v
                own_bf[(q + 1) % 2, at, cols] = v_bf
            else:
                edge_f[edge_slot, c, at] = v
                edge_b[edge_slot, c, at] = v_bf
        if q == STEPS - 1:
            @pl.when(t < n_sub_epochs - 1)
            def _():
                edge_peer(t, c).start()
                edge_own(t, c).start()

            @pl.when(t == n_sub_epochs - 1)
            def _():
                edge_last(t, c).start()
                edge_end(t, c).start()

    def sub_epoch(t, carry):
        @pl.when((t > 0) & (t < n_blk))
        def _():
            for copy in load(t, 0):
                copy.wait()
        for core, order in enumerate(ORDERS):
            @pl.when(lax.rem(blk, 2) == core)
            def _():
                for q in range(STEPS):
                    for op in order:
                        c = int(op[1:] or 0)
                        if op[0] == 'A':
                            send_part(t, q, c)
                        elif op[0] == 'D' and q > 0:
                            step_items(t, q - 1, c)
                        elif op[0] == 'B':
                            own_part(t, q)
                        elif op[0] == 'C':
                            step_items(t, q, c)
                        elif op[0] == 'M':
                            step_users(t, q)
                for op in order:
                    if op[0] == 'D':
                        step_items(t, STEPS - 1, int(op[1:]))
        return carry

    lax.fori_loop(0, n_sub_epochs, sub_epoch, 0)

    u_back = pltpu.make_async_copy(users, u_out, uv_sem.at[0])
    u_back.start()
    end = n_sub_epochs - 1
    last_k = STEPS * n_sub_epochs - 1
    for c in range(n_chunks):
        edge_end(end, c).wait_recv()
        edge_last(end, c).wait_recv()
    for c in range(n_chunks):
        for p in range(PIECES):
            part_copy(last_k - 1, 0, c, p).wait_send()
            part_copy(last_k, 1, c, p).wait_send()
            for q in range(STEPS - 1):
                item_copy(STEPS * end + q, q, c, p).wait_send()
        edge_own(end - 1, c).wait_send()
        edge_peer(end - 1, c).wait_send()
        edge_end(end, c).wait_send()
        edge_last(end, c).wait_send()
    u_back.wait()


def solution(mesh):
    n_blk = mesh.shape['blk']
    n_sub = mesh.shape['sub']
    row_spec = P(('rep', 'blk', 'sub'), None)
    item_spec = P(('rep', 'blk'), None)

    def local_run(ratings, mask, user_init, item_init):
        n_users = ratings.shape[0]
        n_items, rank = item_init.shape
        half = n_items // n_sub
        n_chunks = half // CHUNK
        n_sub_epochs = EPOCHS * n_blk
        n_steps = STEPS * n_sub_epochs
        wide = 128
        big_side = max(n_items, n_sub * n_users)
        eta = STEP_GAIN * math.sqrt(rank) / (math.sqrt(big_side) + math.sqrt(rank)) ** 2
        lam = DECAY / eta
        f32, bf16 = jnp.float32, jnp.bfloat16
        dma = pltpu.SemaphoreType.DMA
        chunk = (rank, CHUNK)
        any_space = pl.BlockSpec(memory_space=pl.ANY)
        users_t, items_t = pl.pallas_call(
            functools.partial(run, n_blk, eta, lam),
            out_shape=[jax.ShapeDtypeStruct((rank, n_users), f32), jax.ShapeDtypeStruct((rank, n_items), f32)],
            in_specs=[pl.BlockSpec(memory_space=pltpu.HBM)] * 4,
            out_specs=[any_space] * 2,
            scratch_shapes=[
                pltpu.VMEM((n_blk, 2, n_users, half), f32),
                pltpu.VMEM((n_blk, 2, n_users, half), jnp.int32),
                pltpu.VMEM((2, n_users, half), bf16),
                pltpu.VMEM((rank, n_users), f32),
                pltpu.VMEM((n_users, wide), bf16),
                pltpu.VMEM((rank, n_users), bf16),
                pltpu.VMEM((rank, half), f32),
                pltpu.VMEM((2, rank, half), bf16),
                pltpu.VMEM((STEPS - 1, n_chunks) + chunk, bf16),
                pltpu.VMEM((rank, half), f32),
                pltpu.VMEM((2, n_chunks) + chunk, f32),
                pltpu.VMEM((n_steps, n_chunks) + chunk, f32),
                pltpu.VMEM((n_steps + 1, n_chunks) + chunk, bf16),
                pltpu.VMEM((n_sub_epochs, n_chunks) + chunk, f32),
                pltpu.VMEM((rank, n_items), f32),
                pltpu.VMEM((2, n_chunks) + chunk, f32),
                pltpu.VMEM((2, n_chunks) + chunk, bf16),
                dma((n_blk, 2, 2)),
                dma((2,)),
                dma((2, n_chunks, PIECES)),
                dma((2, n_chunks, PIECES)),
                dma((STEPS - 1, n_chunks, PIECES)),
                dma((n_chunks, PIECES)),
                dma((2, n_chunks)),
                dma((n_sub_epochs, n_chunks)),
                dma((2, n_chunks)),
                dma((n_sub_epochs, n_chunks)),
                dma((n_chunks,)),
                dma((n_chunks,)),
            ],
            compiler_params=pltpu.CompilerParams(
                collective_id=0, has_side_effects=True, vmem_limit_bytes=52_000_000),
        )(ratings, mask, user_init.T, item_init.T)
        return users_t.T, items_t.T

    return jax.shard_map(local_run, mesh=mesh, in_specs=(row_spec, row_spec, row_spec, item_spec), out_specs=(row_spec, item_spec), check_vma=False)
```

```python
import functools
import math

import jax
import jax.numpy as jnp
from jax import lax
from jax.experimental import pallas as pl
from jax.experimental.pallas import tpu as pltpu
from jax.sharding import PartitionSpec as P

STEPS = 4
EPOCHS = 2
STEP_GAIN = 0.4
DECAY = 0.002
CHUNK = 128
ROWS = 256
PIECES = 2
ORDERS = (
    ('A0', 'B1', 'A1', 'B0', 'A2', 'A3', 'C0', 'M', 'C1', 'C2', 'C3'),
    ('A0', 'A1', 'D2', 'D3', 'B0', 'C0', 'B1', 'A2', 'C1', 'A3', 'M'),
)
MESH = pl.DeviceIdType.MESH
NT = (((1,), (1,)), ((), ()))


def run(n_blk, eta, lam, r_hbm, m_hbm, u_hbm, v_hbm, u_out, v_out,
        rate, known, err, users, users_bf, users_t, own, own_bf, own_next, part, send_p, recv_p,
        peer_v, in_v, v_start, edge_f, edge_b,
        load_sem, uv_sem, p_send, p_recv, v_send, v_recv,
        ef_send, ef_recv, eb_send, eb_recv, el_send, el_recv):
    rank, n_users = users.shape
    half = own.shape[1]
    n_chunks = half // CHUNK
    n_sub_epochs = EPOCHS * n_blk
    pad = users_bf.shape[1] - rank
    me = lax.axis_index('sub')
    other = 1 - me
    blk = lax.axis_index('blk')
    down = lax.rem(blk + n_blk - 1, n_blk)
    up = lax.rem(blk + 1, n_blk)

    def load(t, role):
        owner = me if role else other
        col = pl.multiple_of(lax.rem(blk + t, n_blk) * (2 * half) + owner * half, half)
        return [
            pltpu.make_async_copy(src.at[:, pl.ds(col, half)], dst.at[t, role], load_sem.at[t, role, j])
            for j, (src, dst) in enumerate(((r_hbm, rate), (m_hbm, known)))
        ]

    def start_load(t):
        for role in range(2):
            for copy in load(t, role):
                copy.start()

    u_copy = pltpu.make_async_copy(u_hbm, users, uv_sem.at[0])
    v_copy = pltpu.make_async_copy(v_hbm, v_start, uv_sem.at[1])
    u_copy.start()
    v_copy.start()
    for copy in load(0, 0):
        copy.start()

    barrier = pltpu.get_barrier_semaphore()
    friends = [(blk, other), (down, me), (down, other), (up, me), (up, other)]
    for b, s in friends:
        pl.semaphore_signal(barrier, inc=1, device_id={'sub': s, 'blk': b}, device_id_type=MESH)

    def refresh_users(u):
        u_bf = u.astype(jnp.bfloat16)
        users_t[...] = u_bf
        wide = jnp.concatenate([u, jnp.zeros((pad, n_users), jnp.float32)], axis=0)
        users_bf[...] = wide.T.astype(jnp.bfloat16)

    u_copy.wait()
    refresh_users(users[...])
    v_copy.wait()

    def mine(c):
        return pl.ds(pl.multiple_of(me * half + c * CHUNK, CHUNK), CHUNK)

    for c in range(n_chunks):
        theirs = pl.ds(pl.multiple_of(other * half + c * CHUNK, CHUNK), CHUNK)
        in_v[0, c] = v_start[:, mine(c)]
        peer_v[0, c] = v_start[:, theirs].astype(jnp.bfloat16)
    for copy in load(0, 0):
        copy.wait()
    for copy in load(0, 1):
        copy.start()
    pl.semaphore_wait(barrier, len(friends))

    def remote(src, dst, send, recv, s, b):
        return pltpu.make_async_remote_copy(
            src_ref=src, dst_ref=dst, send_sem=send, recv_sem=recv,
            device_id={'sub': s, 'blk': b}, device_id_type=MESH)

    piece = rank // PIECES

    def part_copy(k, slot, c, p):
        at = pl.ds(p * piece, piece)
        return remote(send_p.at[slot, c, at], recv_p.at[k, c, at], p_send.at[slot, c, p], p_recv.at[slot, c, p], other, blk)

    def item_copy(k, q, c, p):
        at = pl.ds(p * piece, piece)
        return remote(own_next.at[q, c, at], peer_v.at[k + 1, c, at], v_send.at[q, c, p], v_recv.at[c, p], other, blk)

    def edge_own(t, c):
        slot = lax.rem(t, 2)
        return remote(edge_f.at[slot, c], in_v.at[t + 1, c], ef_send.at[slot, c], ef_recv.at[t, c], me, down)

    def edge_peer(t, c):
        slot = lax.rem(t, 2)
        return remote(edge_b.at[slot, c], peer_v.at[STEPS * (t + 1), c], eb_send.at[slot, c], eb_recv.at[t, c], other, down)

    def edge_last(t, c):
        slot = lax.rem(t, 2)
        return remote(edge_f.at[slot, c], v_out.at[:, mine(c)], el_send.at[c], el_recv.at[c], other, down)

    def edge_end(t, c):
        slot = lax.rem(t, 2)
        return remote(edge_f.at[slot, c], v_out.at[:, mine(c)], ef_send.at[slot, c], ef_recv.at[t, c], me, down)

    def widen(v):
        return jnp.concatenate([v, jnp.zeros((pad, v.shape[1]), v.dtype)], axis=0)

    def errors(tm, role, cols, v_bf):
        v_wide = widen(v_bf)
        for r in range(0, n_users, ROWS):
            rows = pl.ds(r, ROWS)
            pred = jnp.dot(users_bf[rows, :], v_wide, preferred_element_type=jnp.float32)
            diff = jnp.where(known[tm, role, rows, cols] != 0, pred - rate[tm, role, rows, cols], 0.0)
            err[role, rows, cols] = diff.astype(jnp.bfloat16)

    def send_part(t, q, c):
        k, slot = STEPS * t + q, q % 2
        if q == 0:
            @pl.when(t > 0)
            def _():
                edge_peer(t - 1, c).wait_recv()
        else:
            for p in range(PIECES):
                item_copy(k - 1, q - 1, c, p).wait_recv()
        cols = pl.ds(c * CHUNK, CHUNK)
        errors(lax.rem(t, n_blk), 0, cols, peer_v[k, c])
        total = jnp.dot(users_t[...], err[0, :, cols], preferred_element_type=jnp.float32)
        for p in range(PIECES):
            if q < 2:
                @pl.when(t > 0)
                def _():
                    part_copy(k - 2, slot, c, p).wait_send()
            else:
                part_copy(k - 2, slot, c, p).wait_send()
        send_p[slot, c] = total
        for p in range(PIECES):
            part_copy(k, slot, c, p).start()

    def own_part(t, q, part_idx, first):
        if q == 0:
            if first:
                @pl.when(t + 1 < n_blk)
                def _():
                    start_load(t + 1)

                @pl.when(t < n_blk)
                def _():
                    for copy in load(t, 1):
                        copy.wait()
            for c in range(part_idx * n_chunks // 2, (part_idx + 1) * n_chunks // 2):
                @pl.when(t > 0)
                def _():
                    edge_own(t - 1, c).wait_recv()
                v = in_v[t, c]
                own[:, pl.ds(c * CHUNK, CHUNK)] = v
                own_bf[0, :, pl.ds(c * CHUNK, CHUNK)] = v.astype(jnp.bfloat16)
        cols = pl.ds(part_idx * half // 2, half // 2)
        errors(lax.rem(t, n_blk), 1, cols, own_bf[q % 2, :, cols])
        part[:, cols] = jnp.dot(users_t[...], err[1, :, cols], preferred_element_type=jnp.float32)

    def step_users(t, q):
        k = STEPS * t + q
        v_peer = jnp.concatenate([peer_v[k, c] for c in range(n_chunks)], axis=1)
        v_own = own_bf[q % 2]
        for r in range(0, n_users, ROWS):
            rows = pl.ds(r, ROWS)
            grad = lax.dot_general(v_peer, err[0, rows, :], NT, preferred_element_type=jnp.float32)
            grad += lax.dot_general(v_own, err[1, rows, :], NT, preferred_element_type=jnp.float32)
            u = users[:, rows]
            users[:, rows] = u - eta * (grad + lam * u)
        refresh_users(users[...])

    def step_items(t, q, c):
        k, slot = STEPS * t + q, q % 2
        cols = pl.ds(c * CHUNK, CHUNK)
        edge_slot = lax.rem(t, 2)
        if q < STEPS - 1:
            @pl.when(t > 0)
            def _():
                for p in range(PIECES):
                    item_copy(k - STEPS, q, c, p).wait_send()
        else:
            @pl.when(t > 1)
            def _():
                edge_own(t - 2, c).wait_send()
                edge_peer(t - 2, c).wait_send()
        for p in range(PIECES):
            at = pl.ds(p * piece, piece)
            part_copy(k, slot, c, p).wait_recv()
            v = own[at, cols]
            v = v - eta * ((part[at, cols] + recv_p[k, c, at]) + lam * v)
            v_bf = v.astype(jnp.bfloat16)
            if q < STEPS - 1:
                own_next[q, c, at] = v_bf
                item_copy(k, q, c, p).start()
                own[at, cols] = v
                own_bf[(q + 1) % 2, at, cols] = v_bf
            else:
                edge_f[edge_slot, c, at] = v
                edge_b[edge_slot, c, at] = v_bf
        if q == STEPS - 1:
            @pl.when(t < n_sub_epochs - 1)
            def _():
                edge_peer(t, c).start()
                edge_own(t, c).start()

            @pl.when(t == n_sub_epochs - 1)
            def _():
                edge_last(t, c).start()
                edge_end(t, c).start()

    def sub_epoch(t, carry):
        @pl.when((t > 0) & (t < n_blk))
        def _():
            for copy in load(t, 0):
                copy.wait()
        for core, order in enumerate(ORDERS):
            @pl.when(lax.rem(blk, 2) == core)
            def _():
                for q in range(STEPS):
                    for op in order:
                        c = int(op[1:] or 0)
                        if op[0] == 'A':
                            send_part(t, q, c)
                        elif op[0] == 'D' and q > 0:
                            step_items(t, q - 1, c)
                        elif op[0] == 'B':
                            own_part(t, q, c, op == next(x for x in order if x[0] == 'B'))
                        elif op[0] == 'C':
                            step_items(t, q, c)
                        elif op[0] == 'M':
                            step_users(t, q)
                for op in order:
                    if op[0] == 'D':
                        step_items(t, STEPS - 1, int(op[1:]))
        return carry

    lax.fori_loop(0, n_sub_epochs, sub_epoch, 0)

    u_back = pltpu.make_async_copy(users, u_out, uv_sem.at[0])
    u_back.start()
    end = n_sub_epochs - 1
    last_k = STEPS * n_sub_epochs - 1
    for c in range(n_chunks):
        edge_end(end, c).wait_recv()
        edge_last(end, c).wait_recv()
    for c in range(n_chunks):
        for p in range(PIECES):
            part_copy(last_k - 1, 0, c, p).wait_send()
            part_copy(last_k, 1, c, p).wait_send()
            for q in range(STEPS - 1):
                item_copy(STEPS * end + q, q, c, p).wait_send()
        edge_own(end - 1, c).wait_send()
        edge_peer(end - 1, c).wait_send()
        edge_end(end, c).wait_send()
        edge_last(end, c).wait_send()
    u_back.wait()


def solution(mesh):
    n_blk = mesh.shape['blk']
    n_sub = mesh.shape['sub']
    row_spec = P(('rep', 'blk', 'sub'), None)
    item_spec = P(('rep', 'blk'), None)

    def local_run(ratings, mask, user_init, item_init):
        n_users = ratings.shape[0]
        n_items, rank = item_init.shape
        half = n_items // n_sub
        n_chunks = half // CHUNK
        n_sub_epochs = EPOCHS * n_blk
        n_steps = STEPS * n_sub_epochs
        wide = 128
        big_side = max(n_items, n_sub * n_users)
        eta = STEP_GAIN * math.sqrt(rank) / (math.sqrt(big_side) + math.sqrt(rank)) ** 2
        lam = DECAY / eta
        f32, bf16 = jnp.float32, jnp.bfloat16
        dma = pltpu.SemaphoreType.DMA
        chunk = (rank, CHUNK)
        any_space = pl.BlockSpec(memory_space=pl.ANY)
        in_hbm = functools.partial(pltpu.with_memory_space_constraint, memory_space=pltpu.HBM)
        users_t, items_t = pl.pallas_call(
            functools.partial(run, n_blk, eta, lam),
            out_shape=[jax.ShapeDtypeStruct((rank, n_users), f32), jax.ShapeDtypeStruct((rank, n_items), f32)],
            in_specs=[any_space] * 4,
            out_specs=[any_space] * 2,
            scratch_shapes=[
                pltpu.VMEM((n_blk, 2, n_users, half), f32),
                pltpu.VMEM((n_blk, 2, n_users, half), jnp.int32),
                pltpu.VMEM((2, n_users, half), bf16),
                pltpu.VMEM((rank, n_users), f32),
                pltpu.VMEM((n_users, wide), bf16),
                pltpu.VMEM((rank, n_users), bf16),
                pltpu.VMEM((rank, half), f32),
                pltpu.VMEM((2, rank, half), bf16),
                pltpu.VMEM((STEPS - 1, n_chunks) + chunk, bf16),
                pltpu.VMEM((rank, half), f32),
                pltpu.VMEM((2, n_chunks) + chunk, f32),
                pltpu.VMEM((n_steps, n_chunks) + chunk, f32),
                pltpu.VMEM((n_steps + 1, n_chunks) + chunk, bf16),
                pltpu.VMEM((n_sub_epochs, n_chunks) + chunk, f32),
                pltpu.VMEM((rank, n_items), f32),
                pltpu.VMEM((2, n_chunks) + chunk, f32),
                pltpu.VMEM((2, n_chunks) + chunk, bf16),
                dma((n_blk, 2, 2)),
                dma((2,)),
                dma((2, n_chunks, PIECES)),
                dma((2, n_chunks, PIECES)),
                dma((STEPS - 1, n_chunks, PIECES)),
                dma((n_chunks, PIECES)),
                dma((2, n_chunks)),
                dma((n_sub_epochs, n_chunks)),
                dma((2, n_chunks)),
                dma((n_sub_epochs, n_chunks)),
                dma((n_chunks,)),
                dma((n_chunks,)),
            ],
            compiler_params=pltpu.CompilerParams(
                collective_id=0, has_side_effects=True, vmem_limit_bytes=52_000_000),
        )(ratings, mask, in_hbm(user_init.T), in_hbm(item_init.T))
        return users_t.T, items_t.T

    return jax.shard_map(local_run, mesh=mesh, in_specs=(row_spec, row_spec, row_spec, item_spec), out_specs=(row_spec, item_spec), check_vma=False)
```

```python
import functools
import math

import jax
import jax.numpy as jnp
from jax import lax
from jax.experimental import pallas as pl
from jax.experimental.pallas import tpu as pltpu
from jax.sharding import PartitionSpec as P

STEPS = 4
EPOCHS = 2
STEP_GAIN = 0.4
DECAY = 0.002
CHUNK = 128
ROWS = 256
PIECES = 2
ORDERS = (
    ('A0', 'A1', 'A2', 'A3', 'B', 'C0', 'M', 'C1', 'C2', 'C3'),
    ('A0', 'A1', 'D2', 'D3', 'B', 'C0', 'A2', 'C1', 'A3', 'M'),
)
MESH = pl.DeviceIdType.MESH
NT = (((1,), (1,)), ((), ()))


def run(n_blk, eta, lam, r_hbm, m_hbm, u_hbm, v_hbm, u_out, v_out,
        rate, known, err, users, users_bf, users_t, own, own_bf, own_next, part, send_p, recv_p,
        peer_v, in_v, v_start, edge_f, edge_b,
        load_sem, uv_sem, p_send, p_recv, v_send, v_recv,
        ef_send, ef_recv, eb_send, eb_recv, el_send, el_recv):
    rank, n_users = users.shape
    half = own.shape[1]
    n_chunks = half // CHUNK
    n_sub_epochs = EPOCHS * n_blk
    pad = users_bf.shape[1] - rank
    me = lax.axis_index('sub')
    other = 1 - me
    blk = lax.axis_index('blk')
    down = lax.rem(blk + n_blk - 1, n_blk)
    up = lax.rem(blk + 1, n_blk)

    def load(t, role):
        owner = me if role else other
        col = pl.multiple_of(lax.rem(blk + t, n_blk) * (2 * half) + owner * half, half)
        return [
            pltpu.make_async_copy(src.at[:, pl.ds(col, half)], dst.at[t, role], load_sem.at[t, role, j])
            for j, (src, dst) in enumerate(((r_hbm, rate), (m_hbm, known)))
        ]

    def start_load(t):
        for role in range(2):
            for copy in load(t, role):
                copy.start()

    u_copy = pltpu.make_async_copy(u_hbm, users, uv_sem.at[0])
    v_copy = pltpu.make_async_copy(v_hbm, v_start, uv_sem.at[1])
    u_copy.start()
    v_copy.start()
    for copy in load(0, 0):
        copy.start()

    barrier = pltpu.get_barrier_semaphore()
    friends = [(blk, other), (down, me), (down, other), (up, me), (up, other)]
    for b, s in friends:
        pl.semaphore_signal(barrier, inc=1, device_id={'sub': s, 'blk': b}, device_id_type=MESH)

    def refresh_users(u):
        u_bf = u.astype(jnp.bfloat16)
        users_t[...] = u_bf
        wide = jnp.concatenate([u, jnp.zeros((pad, n_users), jnp.float32)], axis=0)
        users_bf[...] = wide.T.astype(jnp.bfloat16)

    u_copy.wait()
    refresh_users(users[...])
    v_copy.wait()

    def mine(c):
        return pl.ds(pl.multiple_of(me * half + c * CHUNK, CHUNK), CHUNK)

    for c in range(n_chunks):
        theirs = pl.ds(pl.multiple_of(other * half + c * CHUNK, CHUNK), CHUNK)
        in_v[0, c] = v_start[:, mine(c)]
        peer_v[0, c] = v_start[:, theirs].astype(jnp.bfloat16)
    for copy in load(0, 0):
        copy.wait()
    for copy in load(0, 1):
        copy.start()
    pl.semaphore_wait(barrier, len(friends))

    def remote(src, dst, send, recv, s, b):
        return pltpu.make_async_remote_copy(
            src_ref=src, dst_ref=dst, send_sem=send, recv_sem=recv,
            device_id={'sub': s, 'blk': b}, device_id_type=MESH)

    piece = rank // PIECES

    def part_copy(k, slot, c, p):
        at = pl.ds(p * piece, piece)
        return remote(send_p.at[slot, c, at], recv_p.at[k, c, at], p_send.at[slot, c, p], p_recv.at[slot, c, p], other, blk)

    def item_copy(k, q, c, p):
        at = pl.ds(p * piece, piece)
        return remote(own_next.at[q, c, at], peer_v.at[k + 1, c, at], v_send.at[q, c, p], v_recv.at[c, p], other, blk)

    def edge_own(t, c):
        slot = lax.rem(t, 2)
        return remote(edge_f.at[slot, c], in_v.at[t + 1, c], ef_send.at[slot, c], ef_recv.at[t, c], me, down)

    def edge_peer(t, c):
        slot = lax.rem(t, 2)
        return remote(edge_b.at[slot, c], peer_v.at[STEPS * (t + 1), c], eb_send.at[slot, c], eb_recv.at[t, c], other, down)

    def edge_last(t, c):
        slot = lax.rem(t, 2)
        return remote(edge_f.at[slot, c], v_out.at[:, mine(c)], el_send.at[c], el_recv.at[c], other, down)

    def edge_end(t, c):
        slot = lax.rem(t, 2)
        return remote(edge_f.at[slot, c], v_out.at[:, mine(c)], ef_send.at[slot, c], ef_recv.at[t, c], me, down)

    def widen(v):
        return jnp.concatenate([v, jnp.zeros((pad, v.shape[1]), v.dtype)], axis=0)

    def errors(tm, role, cols, v_bf):
        v_wide = widen(v_bf)
        for r in range(0, n_users, ROWS):
            rows = pl.ds(r, ROWS)
            pred = jnp.dot(users_bf[rows, :], v_wide, preferred_element_type=jnp.float32)
            diff = jnp.where(known[tm, role, rows, cols] != 0, pred - rate[tm, role, rows, cols], 0.0)
            err[role, rows, cols] = diff.astype(jnp.bfloat16)

    def send_part(t, q, c):
        k, slot = STEPS * t + q, q % 2
        if q == 0:
            @pl.when(t > 0)
            def _():
                edge_peer(t - 1, c).wait_recv()
        else:
            for p in range(PIECES):
                item_copy(k - 1, q - 1, c, p).wait_recv()
        cols = pl.ds(c * CHUNK, CHUNK)
        errors(lax.rem(t, n_blk), 0, cols, peer_v[k, c])
        total = jnp.dot(users_t[...], err[0, :, cols], preferred_element_type=jnp.float32)
        for p in range(PIECES):
            if q < 2:
                @pl.when(t > 0)
                def _():
                    part_copy(k - 2, slot, c, p).wait_send()
            else:
                part_copy(k - 2, slot, c, p).wait_send()
        send_p[slot, c] = total
        for p in range(PIECES):
            part_copy(k, slot, c, p).start()

    def own_part(t, q):
        if q == 0:
            @pl.when(t + 1 < n_blk)
            def _():
                start_load(t + 1)

            @pl.when(t < n_blk)
            def _():
                for copy in load(t, 1):
                    copy.wait()
            for c in range(n_chunks):
                @pl.when(t > 0)
                def _():
                    edge_own(t - 1, c).wait_recv()
                v = in_v[t, c]
                own[:, pl.ds(c * CHUNK, CHUNK)] = v
                own_bf[0, :, pl.ds(c * CHUNK, CHUNK)] = v.astype(jnp.bfloat16)
        for c in range(0, half, 256):
            cols = pl.ds(c, 256)
            errors(lax.rem(t, n_blk), 1, cols, own_bf[q % 2, :, cols])
            part[:, cols] = jnp.dot(users_t[...], err[1, :, cols], preferred_element_type=jnp.float32)

    def step_users(t, q):
        k = STEPS * t + q
        v_peer = jnp.concatenate([peer_v[k, c] for c in range(n_chunks)], axis=1)
        v_own = own_bf[q % 2]
        for r in range(0, n_users, ROWS):
            rows = pl.ds(r, ROWS)
            grad = lax.dot_general(v_peer, err[0, rows, :], NT, preferred_element_type=jnp.float32)
            grad += lax.dot_general(v_own, err[1, rows, :], NT, preferred_element_type=jnp.float32)
            u = users[:, rows]
            users[:, rows] = u - eta * (grad + lam * u)
        refresh_users(users[...])

    def step_items(t, q, c):
        k, slot = STEPS * t + q, q % 2
        cols = pl.ds(c * CHUNK, CHUNK)
        edge_slot = lax.rem(t, 2)
        if q < STEPS - 1:
            @pl.when(t > 0)
            def _():
                for p in range(PIECES):
                    item_copy(k - STEPS, q, c, p).wait_send()
        else:
            @pl.when(t > 1)
            def _():
                edge_own(t - 2, c).wait_send()
                edge_peer(t - 2, c).wait_send()
        for p in range(PIECES):
            at = pl.ds(p * piece, piece)
            part_copy(k, slot, c, p).wait_recv()
            v = own[at, cols]
            v = v - eta * ((part[at, cols] + recv_p[k, c, at]) + lam * v)
            v_bf = v.astype(jnp.bfloat16)
            if q < STEPS - 1:
                own_next[q, c, at] = v_bf
                item_copy(k, q, c, p).start()
                own[at, cols] = v
                own_bf[(q + 1) % 2, at, cols] = v_bf
            else:
                edge_f[edge_slot, c, at] = v
                edge_b[edge_slot, c, at] = v_bf
        if q == STEPS - 1:
            @pl.when(t < n_sub_epochs - 1)
            def _():
                edge_peer(t, c).start()
                edge_own(t, c).start()

            @pl.when(t == n_sub_epochs - 1)
            def _():
                edge_last(t, c).start()
                edge_end(t, c).start()

    def sub_epoch(t, carry):
        @pl.when((t > 0) & (t < n_blk))
        def _():
            for copy in load(t, 0):
                copy.wait()
        for core, order in enumerate(ORDERS):
            @pl.when(lax.rem(blk, 2) == core)
            def _():
                for q in range(STEPS):
                    for op in order:
                        c = int(op[1:] or 0)
                        if op[0] == 'A':
                            send_part(t, q, c)
                        elif op[0] == 'D' and q > 0:
                            step_items(t, q - 1, c)
                        elif op[0] == 'B':
                            own_part(t, q)
                        elif op[0] == 'C':
                            step_items(t, q, c)
                        elif op[0] == 'M':
                            step_users(t, q)
                for op in order:
                    if op[0] == 'D':
                        step_items(t, STEPS - 1, int(op[1:]))
        return carry

    lax.fori_loop(0, n_sub_epochs, sub_epoch, 0)

    u_back = pltpu.make_async_copy(users, u_out, uv_sem.at[0])
    u_back.start()
    end = n_sub_epochs - 1
    last_k = STEPS * n_sub_epochs - 1
    for c in range(n_chunks):
        edge_end(end, c).wait_recv()
        edge_last(end, c).wait_recv()
    for c in range(n_chunks):
        for p in range(PIECES):
            part_copy(last_k - 1, 0, c, p).wait_send()
            part_copy(last_k, 1, c, p).wait_send()
            for q in range(STEPS - 1):
                item_copy(STEPS * end + q, q, c, p).wait_send()
        edge_own(end - 1, c).wait_send()
        edge_peer(end - 1, c).wait_send()
        edge_end(end, c).wait_send()
        edge_last(end, c).wait_send()
    u_back.wait()


def solution(mesh):
    n_blk = mesh.shape['blk']
    n_sub = mesh.shape['sub']
    row_spec = P(('rep', 'blk', 'sub'), None)
    item_spec = P(('rep', 'blk'), None)

    def local_run(ratings, mask, user_init, item_init):
        n_users = ratings.shape[0]
        n_items, rank = item_init.shape
        half = n_items // n_sub
        n_chunks = half // CHUNK
        n_sub_epochs = EPOCHS * n_blk
        n_steps = STEPS * n_sub_epochs
        wide = 128
        big_side = max(n_items, n_sub * n_users)
        eta = STEP_GAIN * math.sqrt(rank) / (math.sqrt(big_side) + math.sqrt(rank)) ** 2
        lam = DECAY / eta
        f32, bf16 = jnp.float32, jnp.bfloat16
        dma = pltpu.SemaphoreType.DMA
        chunk = (rank, CHUNK)
        any_space = pl.BlockSpec(memory_space=pl.ANY)
        in_hbm = functools.partial(pltpu.with_memory_space_constraint, memory_space=pltpu.HBM)
        users_t, items_t = pl.pallas_call(
            functools.partial(run, n_blk, eta, lam),
            out_shape=[jax.ShapeDtypeStruct((rank, n_users), f32), jax.ShapeDtypeStruct((rank, n_items), f32)],
            in_specs=[any_space] * 4,
            out_specs=[any_space] * 2,
            scratch_shapes=[
                pltpu.VMEM((n_blk, 2, n_users, half), f32),
                pltpu.VMEM((n_blk, 2, n_users, half), jnp.int32),
                pltpu.VMEM((2, n_users, half), bf16),
                pltpu.VMEM((rank, n_users), f32),
                pltpu.VMEM((n_users, wide), bf16),
                pltpu.VMEM((rank, n_users), bf16),
                pltpu.VMEM((rank, half), f32),
                pltpu.VMEM((2, rank, half), bf16),
                pltpu.VMEM((STEPS - 1, n_chunks) + chunk, bf16),
                pltpu.VMEM((rank, half), f32),
                pltpu.VMEM((2, n_chunks) + chunk, f32),
                pltpu.VMEM((n_steps, n_chunks) + chunk, f32),
                pltpu.VMEM((n_steps + 1, n_chunks) + chunk, bf16),
                pltpu.VMEM((n_sub_epochs, n_chunks) + chunk, f32),
                pltpu.VMEM((rank, n_items), f32),
                pltpu.VMEM((2, n_chunks) + chunk, f32),
                pltpu.VMEM((2, n_chunks) + chunk, bf16),
                dma((n_blk, 2, 2)),
                dma((2,)),
                dma((2, n_chunks, PIECES)),
                dma((2, n_chunks, PIECES)),
                dma((STEPS - 1, n_chunks, PIECES)),
                dma((n_chunks, PIECES)),
                dma((2, n_chunks)),
                dma((n_sub_epochs, n_chunks)),
                dma((2, n_chunks)),
                dma((n_sub_epochs, n_chunks)),
                dma((n_chunks,)),
                dma((n_chunks,)),
            ],
            compiler_params=pltpu.CompilerParams(
                collective_id=0, has_side_effects=True, vmem_limit_bytes=52_000_000),
        )(ratings, mask, in_hbm(user_init.T), in_hbm(item_init.T))
        return users_t.T, items_t.T

    return jax.shard_map(local_run, mesh=mesh, in_specs=(row_spec, row_spec, row_spec, item_spec), out_specs=(row_spec, item_spec), check_vma=False)
```

```python
import functools
import math

import jax
import jax.numpy as jnp
from jax import lax
from jax.experimental import pallas as pl
from jax.experimental.pallas import tpu as pltpu
from jax.sharding import PartitionSpec as P

STEPS = 4
EPOCHS = 2
STEP_GAIN = 0.4
DECAY = 0.002
CHUNK = 128
ROWS = 256
PIECES = 2
MIDDLE = ('A0', 'A1', 'D2', 'D3', 'B', 'C0', 'A2', 'C1', 'A3', 'M')
ORDERS = (
    (
        ('A0', 'A1', 'B', 'A2', 'A3', 'C0', 'C1', 'M', 'C2', 'C3'),
        ('A0', 'B', 'A1', 'A2', 'A3', 'C0', 'M', 'C1', 'C2', 'C3'),
        ('A0', 'B', 'A1', 'A2', 'A3', 'C0', 'M', 'C1', 'C2', 'C3'),
        ('A0', 'A1', 'A2', 'A3', 'B', 'C0', 'C1', 'M', 'C2', 'C3'),
    ),
    (
        ('A0', 'A1', 'B', 'C0', 'A2', 'C1', 'A3', 'M'),
        MIDDLE,
        MIDDLE,
        ('A0', 'A1', 'D2', 'D3', 'B', 'C0', 'A2', 'A3', 'C1', 'M', 'C2', 'C3'),
    ),
)
MESH = pl.DeviceIdType.MESH
NT = (((1,), (1,)), ((), ()))


def run(n_blk, eta, lam, r_hbm, m_hbm, u_hbm, v_hbm, u_out, v_out,
        rate, known, err, users, users_bf, users_t, own, own_bf, own_next, part, send_p, recv_p,
        peer_v, in_v, v_start, edge_f, edge_b,
        load_sem, uv_sem, p_send, p_recv, v_send, v_recv,
        ef_send, ef_recv, eb_send, eb_recv, el_send, el_recv):
    rank, n_users = users.shape
    half = own.shape[1]
    n_chunks = half // CHUNK
    n_sub_epochs = EPOCHS * n_blk
    pad = users_bf.shape[1] - rank
    me = lax.axis_index('sub')
    other = 1 - me
    blk = lax.axis_index('blk')
    down = lax.rem(blk + n_blk - 1, n_blk)
    up = lax.rem(blk + 1, n_blk)

    def load(t, role):
        owner = me if role else other
        col = pl.multiple_of(lax.rem(blk + t, n_blk) * (2 * half) + owner * half, half)
        return [
            pltpu.make_async_copy(src.at[:, pl.ds(col, half)], dst.at[t, role], load_sem.at[t, role, j])
            for j, (src, dst) in enumerate(((r_hbm, rate), (m_hbm, known)))
        ]

    def start_load(t):
        for role in range(2):
            for copy in load(t, role):
                copy.start()

    u_copy = pltpu.make_async_copy(u_hbm, users, uv_sem.at[0])
    v_copy = pltpu.make_async_copy(v_hbm, v_start, uv_sem.at[1])
    u_copy.start()
    v_copy.start()
    for copy in load(0, 0):
        copy.start()

    barrier = pltpu.get_barrier_semaphore()
    friends = [(blk, other), (down, me), (down, other), (up, me), (up, other)]
    for b, s in friends:
        pl.semaphore_signal(barrier, inc=1, device_id={'sub': s, 'blk': b}, device_id_type=MESH)

    def refresh_users(u):
        u_bf = u.astype(jnp.bfloat16)
        users_t[...] = u_bf
        wide = jnp.concatenate([u, jnp.zeros((pad, n_users), jnp.float32)], axis=0)
        users_bf[...] = wide.T.astype(jnp.bfloat16)

    u_copy.wait()
    refresh_users(users[...])
    v_copy.wait()

    def mine(c):
        return pl.ds(pl.multiple_of(me * half + c * CHUNK, CHUNK), CHUNK)

    for c in range(n_chunks):
        theirs = pl.ds(pl.multiple_of(other * half + c * CHUNK, CHUNK), CHUNK)
        in_v[0, c] = v_start[:, mine(c)]
        peer_v[0, c] = v_start[:, theirs].astype(jnp.bfloat16)
    for copy in load(0, 0):
        copy.wait()
    for copy in load(0, 1):
        copy.start()
    pl.semaphore_wait(barrier, len(friends))

    def remote(src, dst, send, recv, s, b):
        return pltpu.make_async_remote_copy(
            src_ref=src, dst_ref=dst, send_sem=send, recv_sem=recv,
            device_id={'sub': s, 'blk': b}, device_id_type=MESH)

    piece = rank // PIECES

    def part_copy(k, slot, c, p):
        at = pl.ds(p * piece, piece)
        return remote(send_p.at[slot, c, at], recv_p.at[k, c, at], p_send.at[slot, c, p], p_recv.at[slot, c, p], other, blk)

    def item_copy(k, q, c, p):
        at = pl.ds(p * piece, piece)
        return remote(own_next.at[q, c, at], peer_v.at[k + 1, c, at], v_send.at[q, c, p], v_recv.at[c, p], other, blk)

    def edge_own(t, c):
        slot = lax.rem(t, 2)
        return remote(edge_f.at[slot, c], in_v.at[t + 1, c], ef_send.at[slot, c], ef_recv.at[t, c], me, down)

    def edge_peer(t, c):
        slot = lax.rem(t, 2)
        return remote(edge_b.at[slot, c], peer_v.at[STEPS * (t + 1), c], eb_send.at[slot, c], eb_recv.at[t, c], other, down)

    def edge_last(t, c):
        slot = lax.rem(t, 2)
        return remote(edge_f.at[slot, c], v_out.at[:, mine(c)], el_send.at[c], el_recv.at[c], other, down)

    def edge_end(t, c):
        slot = lax.rem(t, 2)
        return remote(edge_f.at[slot, c], v_out.at[:, mine(c)], ef_send.at[slot, c], ef_recv.at[t, c], me, down)

    def widen(v):
        return jnp.concatenate([v, jnp.zeros((pad, v.shape[1]), v.dtype)], axis=0)

    def errors(tm, role, cols, v_bf):
        v_wide = widen(v_bf)
        for r in range(0, n_users, ROWS):
            rows = pl.ds(r, ROWS)
            pred = jnp.dot(users_bf[rows, :], v_wide, preferred_element_type=jnp.float32)
            diff = jnp.where(known[tm, role, rows, cols] != 0, pred - rate[tm, role, rows, cols], 0.0)
            err[role, rows, cols] = diff.astype(jnp.bfloat16)

    def send_part(t, q, c):
        k, slot = STEPS * t + q, q % 2
        if q == 0:
            @pl.when(t > 0)
            def _():
                edge_peer(t - 1, c).wait_recv()
        else:
            for p in range(PIECES):
                item_copy(k - 1, q - 1, c, p).wait_recv()
        cols = pl.ds(c * CHUNK, CHUNK)
        errors(lax.rem(t, n_blk), 0, cols, peer_v[k, c])
        total = jnp.dot(users_t[...], err[0, :, cols], preferred_element_type=jnp.float32)
        for p in range(PIECES):
            if q < 2:
                @pl.when(t > 0)
                def _():
                    part_copy(k - 2, slot, c, p).wait_send()
            else:
                part_copy(k - 2, slot, c, p).wait_send()
        send_p[slot, c] = total
        for p in range(PIECES):
            part_copy(k, slot, c, p).start()

    def own_part(t, q):
        if q == 0:
            @pl.when(t + 1 < n_blk)
            def _():
                start_load(t + 1)

            @pl.when(t < n_blk)
            def _():
                for copy in load(t, 1):
                    copy.wait()
            for c in range(n_chunks):
                @pl.when(t > 0)
                def _():
                    edge_own(t - 1, c).wait_recv()
                v = in_v[t, c]
                own[:, pl.ds(c * CHUNK, CHUNK)] = v
                own_bf[0, :, pl.ds(c * CHUNK, CHUNK)] = v.astype(jnp.bfloat16)
        for c in range(0, half, 256):
            cols = pl.ds(c, 256)
            errors(lax.rem(t, n_blk), 1, cols, own_bf[q % 2, :, cols])
            part[:, cols] = jnp.dot(users_t[...], err[1, :, cols], preferred_element_type=jnp.float32)

    def step_users(t, q):
        k = STEPS * t + q
        v_peer = jnp.concatenate([peer_v[k, c] for c in range(n_chunks)], axis=1)
        v_own = own_bf[q % 2]
        for r in range(0, n_users, ROWS):
            rows = pl.ds(r, ROWS)
            grad = lax.dot_general(v_peer, err[0, rows, :], NT, preferred_element_type=jnp.float32)
            grad += lax.dot_general(v_own, err[1, rows, :], NT, preferred_element_type=jnp.float32)
            u = users[:, rows]
            users[:, rows] = u - eta * (grad + lam * u)
        refresh_users(users[...])

    def step_items(t, q, c):
        k, slot = STEPS * t + q, q % 2
        cols = pl.ds(c * CHUNK, CHUNK)
        edge_slot = lax.rem(t, 2)
        if q < STEPS - 1:
            @pl.when(t > 0)
            def _():
                for p in range(PIECES):
                    item_copy(k - STEPS, q, c, p).wait_send()
        else:
            @pl.when(t > 1)
            def _():
                edge_own(t - 2, c).wait_send()
                edge_peer(t - 2, c).wait_send()
        for p in range(PIECES):
            at = pl.ds(p * piece, piece)
            part_copy(k, slot, c, p).wait_recv()
            v = own[at, cols]
            v = v - eta * ((part[at, cols] + recv_p[k, c, at]) + lam * v)
            v_bf = v.astype(jnp.bfloat16)
            if q < STEPS - 1:
                own_next[q, c, at] = v_bf
                item_copy(k, q, c, p).start()
                own[at, cols] = v
                own_bf[(q + 1) % 2, at, cols] = v_bf
            else:
                edge_f[edge_slot, c, at] = v
                edge_b[edge_slot, c, at] = v_bf
        if q == STEPS - 1:
            @pl.when(t < n_sub_epochs - 1)
            def _():
                edge_peer(t, c).start()
                edge_own(t, c).start()

            @pl.when(t == n_sub_epochs - 1)
            def _():
                edge_last(t, c).start()
                edge_end(t, c).start()

    def sub_epoch(t, carry):
        @pl.when((t > 0) & (t < n_blk))
        def _():
            for copy in load(t, 0):
                copy.wait()
        for core, orders in enumerate(ORDERS):
            @pl.when(lax.rem(blk, 2) == core)
            def _():
                for q in range(STEPS):
                    for op in orders[q]:
                        c = int(op[1:] or 0)
                        if op[0] == 'A':
                            send_part(t, q, c)
                        elif op[0] == 'B':
                            own_part(t, q)
                        elif op[0] == 'C':
                            step_items(t, q, c)
                        elif op[0] == 'D':
                            step_items(t, q - 1, c)
                        else:
                            step_users(t, q)
        return carry

    lax.fori_loop(0, n_sub_epochs, sub_epoch, 0)

    u_back = pltpu.make_async_copy(users, u_out, uv_sem.at[0])
    u_back.start()
    end = n_sub_epochs - 1
    last_k = STEPS * n_sub_epochs - 1
    for c in range(n_chunks):
        edge_end(end, c).wait_recv()
        edge_last(end, c).wait_recv()
    for c in range(n_chunks):
        for p in range(PIECES):
            part_copy(last_k - 1, 0, c, p).wait_send()
            part_copy(last_k, 1, c, p).wait_send()
            for q in range(STEPS - 1):
                item_copy(STEPS * end + q, q, c, p).wait_send()
        edge_own(end - 1, c).wait_send()
        edge_peer(end - 1, c).wait_send()
        edge_end(end, c).wait_send()
        edge_last(end, c).wait_send()
    u_back.wait()


def solution(mesh):
    n_blk = mesh.shape['blk']
    n_sub = mesh.shape['sub']
    row_spec = P(('rep', 'blk', 'sub'), None)
    item_spec = P(('rep', 'blk'), None)

    def local_run(ratings, mask, user_init, item_init):
        n_users = ratings.shape[0]
        n_items, rank = item_init.shape
        half = n_items // n_sub
        n_chunks = half // CHUNK
        n_sub_epochs = EPOCHS * n_blk
        n_steps = STEPS * n_sub_epochs
        wide = 128
        big_side = max(n_items, n_sub * n_users)
        eta = STEP_GAIN * math.sqrt(rank) / (math.sqrt(big_side) + math.sqrt(rank)) ** 2
        lam = DECAY / eta
        f32, bf16 = jnp.float32, jnp.bfloat16
        dma = pltpu.SemaphoreType.DMA
        chunk = (rank, CHUNK)
        any_space = pl.BlockSpec(memory_space=pl.ANY)
        in_hbm = functools.partial(pltpu.with_memory_space_constraint, memory_space=pltpu.HBM)
        users_t, items_t = pl.pallas_call(
            functools.partial(run, n_blk, eta, lam),
            out_shape=[jax.ShapeDtypeStruct((rank, n_users), f32), jax.ShapeDtypeStruct((rank, n_items), f32)],
            in_specs=[any_space] * 4,
            out_specs=[any_space] * 2,
            scratch_shapes=[
                pltpu.VMEM((n_blk, 2, n_users, half), f32),
                pltpu.VMEM((n_blk, 2, n_users, half), jnp.int32),
                pltpu.VMEM((2, n_users, half), bf16),
                pltpu.VMEM((rank, n_users), f32),
                pltpu.VMEM((n_users, wide), bf16),
                pltpu.VMEM((rank, n_users), bf16),
                pltpu.VMEM((rank, half), f32),
                pltpu.VMEM((2, rank, half), bf16),
                pltpu.VMEM((STEPS - 1, n_chunks) + chunk, bf16),
                pltpu.VMEM((rank, half), f32),
                pltpu.VMEM((2, n_chunks) + chunk, f32),
                pltpu.VMEM((n_steps, n_chunks) + chunk, f32),
                pltpu.VMEM((n_steps + 1, n_chunks) + chunk, bf16),
                pltpu.VMEM((n_sub_epochs, n_chunks) + chunk, f32),
                pltpu.VMEM((rank, n_items), f32),
                pltpu.VMEM((2, n_chunks) + chunk, f32),
                pltpu.VMEM((2, n_chunks) + chunk, bf16),
                dma((n_blk, 2, 2)),
                dma((2,)),
                dma((2, n_chunks, PIECES)),
                dma((2, n_chunks, PIECES)),
                dma((STEPS - 1, n_chunks, PIECES)),
                dma((n_chunks, PIECES)),
                dma((2, n_chunks)),
                dma((n_sub_epochs, n_chunks)),
                dma((2, n_chunks)),
                dma((n_sub_epochs, n_chunks)),
                dma((n_chunks,)),
                dma((n_chunks,)),
            ],
            compiler_params=pltpu.CompilerParams(
                collective_id=0, has_side_effects=True, vmem_limit_bytes=52_000_000),
        )(ratings, mask, in_hbm(user_init.T), in_hbm(item_init.T))
        return users_t.T, items_t.T

    return jax.shard_map(local_run, mesh=mesh, in_specs=(row_spec, row_spec, row_spec, item_spec), out_specs=(row_spec, item_spec), check_vma=False)
```

```python
import functools
import math

import jax
import jax.numpy as jnp
from jax import lax
from jax.experimental import pallas as pl
from jax.experimental.pallas import tpu as pltpu
from jax.sharding import PartitionSpec as P

STEPS = 4
EPOCHS = 2
STEP_GAIN = 0.4
DECAY = 0.002
CHUNK = 128
ROWS = 256
PIECES = 2
ORDERS = (
    ('A0', 'A1', 'A2', 'A3', 'B', 'C0', 'M', 'C1', 'C2', 'C3'),
    ('A0', 'A1', 'D2', 'D3', 'B', 'C0', 'A2', 'C1', 'A3', 'M'),
)
MESH = pl.DeviceIdType.MESH
NT = (((1,), (1,)), ((), ()))


def run(n_blk, eta, lam, r_hbm, m_hbm, u_hbm, v_hbm, u_out, v_out,
        rate, known, err, users, users_bf, users_t, own, own_bf, own_next, part, send_p, recv_p,
        peer_v, in_v, v_start, edge_f, edge_b,
        load_sem, first_sem, uv_sem, p_send, p_recv, v_send, v_recv,
        ef_send, ef_recv, eb_send, eb_recv, el_send, el_recv):
    rank, n_users = users.shape
    half = own.shape[1]
    n_chunks = half // CHUNK
    n_sub_epochs = EPOCHS * n_blk
    pad = users_bf.shape[1] - rank
    me = lax.axis_index('sub')
    other = 1 - me
    blk = lax.axis_index('blk')
    down = lax.rem(blk + n_blk - 1, n_blk)
    up = lax.rem(blk + 1, n_blk)

    def load(t, role):
        owner = me if role else other
        col = pl.multiple_of(lax.rem(blk + t, n_blk) * (2 * half) + owner * half, half)
        return [
            pltpu.make_async_copy(src.at[:, pl.ds(col, half)], dst.at[t, role], load_sem.at[t, role, j])
            for j, (src, dst) in enumerate(((r_hbm, rate), (m_hbm, known)))
        ]

    def first_load(c):
        col = pl.multiple_of(blk * (2 * half) + other * half + c * CHUNK, CHUNK)
        return [
            pltpu.make_async_copy(src.at[:, pl.ds(col, CHUNK)], dst.at[0, 0, :, pl.ds(c * CHUNK, CHUNK)], first_sem.at[c, j])
            for j, (src, dst) in enumerate(((r_hbm, rate), (m_hbm, known)))
        ]

    def start_load(t):
        for role in range(2):
            for copy in load(t, role):
                copy.start()

    u_copy = pltpu.make_async_copy(u_hbm, users, uv_sem.at[0])
    v_copy = pltpu.make_async_copy(v_hbm, v_start, uv_sem.at[1])
    u_copy.start()
    v_copy.start()
    for c in range(n_chunks):
        for copy in first_load(c):
            copy.start()

    barrier = pltpu.get_barrier_semaphore()
    friends = [(blk, other), (down, me), (down, other), (up, me), (up, other)]
    for b, s in friends:
        pl.semaphore_signal(barrier, inc=1, device_id={'sub': s, 'blk': b}, device_id_type=MESH)

    def refresh_users(u):
        u_bf = u.astype(jnp.bfloat16)
        users_t[...] = u_bf
        wide = jnp.concatenate([u, jnp.zeros((pad, n_users), jnp.float32)], axis=0)
        users_bf[...] = wide.T.astype(jnp.bfloat16)

    u_copy.wait()
    refresh_users(users[...])
    v_copy.wait()

    def mine(c):
        return pl.ds(pl.multiple_of(me * half + c * CHUNK, CHUNK), CHUNK)

    for c in range(n_chunks):
        theirs = pl.ds(pl.multiple_of(other * half + c * CHUNK, CHUNK), CHUNK)
        in_v[0, c] = v_start[:, mine(c)]
        peer_v[0, c] = v_start[:, theirs].astype(jnp.bfloat16)
    pl.semaphore_wait(barrier, len(friends))

    def remote(src, dst, send, recv, s, b):
        return pltpu.make_async_remote_copy(
            src_ref=src, dst_ref=dst, send_sem=send, recv_sem=recv,
            device_id={'sub': s, 'blk': b}, device_id_type=MESH)

    piece = rank // PIECES

    def part_copy(k, slot, c, p):
        at = pl.ds(p * piece, piece)
        return remote(send_p.at[slot, c, at], recv_p.at[k, c, at], p_send.at[slot, c, p], p_recv.at[slot, c, p], other, blk)

    def item_copy(k, q, c, p):
        at = pl.ds(p * piece, piece)
        return remote(own_next.at[q, c, at], peer_v.at[k + 1, c, at], v_send.at[q, c, p], v_recv.at[c, p], other, blk)

    def edge_own(t, c):
        slot = lax.rem(t, 2)
        return remote(edge_f.at[slot, c], in_v.at[t + 1, c], ef_send.at[slot, c], ef_recv.at[t, c], me, down)

    def edge_peer(t, c, p):
        slot, at = lax.rem(t, 2), pl.ds(p * piece, piece)
        return remote(edge_b.at[slot, c, at], peer_v.at[STEPS * (t + 1), c, at], eb_send.at[slot, c, p], eb_recv.at[t, c, p], other, down)

    def edge_last(t, c):
        slot = lax.rem(t, 2)
        return remote(edge_f.at[slot, c], v_out.at[:, mine(c)], el_send.at[c], el_recv.at[c], other, down)

    def edge_end(t, c):
        slot = lax.rem(t, 2)
        return remote(edge_f.at[slot, c], v_out.at[:, mine(c)], ef_send.at[slot, c], ef_recv.at[t, c], me, down)

    def widen(v):
        return jnp.concatenate([v, jnp.zeros((pad, v.shape[1]), v.dtype)], axis=0)

    def errors(tm, role, cols, v_bf):
        v_wide = widen(v_bf)
        for r in range(0, n_users, ROWS):
            rows = pl.ds(r, ROWS)
            pred = jnp.dot(users_bf[rows, :], v_wide, preferred_element_type=jnp.float32)
            diff = jnp.where(known[tm, role, rows, cols] != 0, pred - rate[tm, role, rows, cols], 0.0)
            err[role, rows, cols] = diff.astype(jnp.bfloat16)

    def send_part(t, q, c):
        k, slot = STEPS * t + q, q % 2
        if q == 0:
            @pl.when(t == 0)
            def _():
                for copy in first_load(c):
                    copy.wait()
                if c == 1:
                    for copy in load(0, 1):
                        copy.start()

            @pl.when(t > 0)
            def _():
                for p in range(PIECES):
                    edge_peer(t - 1, c, p).wait_recv()
        else:
            for p in range(PIECES):
                item_copy(k - 1, q - 1, c, p).wait_recv()
        cols = pl.ds(c * CHUNK, CHUNK)
        errors(lax.rem(t, n_blk), 0, cols, peer_v[k, c])
        total = jnp.dot(users_t[...], err[0, :, cols], preferred_element_type=jnp.float32)
        for p in range(PIECES):
            if q < 2:
                @pl.when(t > 0)
                def _():
                    part_copy(k - 2, slot, c, p).wait_send()
            else:
                part_copy(k - 2, slot, c, p).wait_send()
        send_p[slot, c] = total
        for p in range(PIECES):
            part_copy(k, slot, c, p).start()

    def own_part(t, q):
        if q == 0:
            @pl.when(t + 1 < n_blk)
            def _():
                start_load(t + 1)

            @pl.when(t < n_blk)
            def _():
                for copy in load(t, 1):
                    copy.wait()
            for c in range(n_chunks):
                @pl.when(t > 0)
                def _():
                    edge_own(t - 1, c).wait_recv()
                v = in_v[t, c]
                own[:, pl.ds(c * CHUNK, CHUNK)] = v
                own_bf[0, :, pl.ds(c * CHUNK, CHUNK)] = v.astype(jnp.bfloat16)
        for c in range(0, half, 256):
            cols = pl.ds(c, 256)
            errors(lax.rem(t, n_blk), 1, cols, own_bf[q % 2, :, cols])
            part[:, cols] = jnp.dot(users_t[...], err[1, :, cols], preferred_element_type=jnp.float32)

    def step_users(t, q):
        k = STEPS * t + q
        v_peer = jnp.concatenate([peer_v[k, c] for c in range(n_chunks)], axis=1)
        v_own = own_bf[q % 2]
        for r in range(0, n_users, ROWS):
            rows = pl.ds(r, ROWS)
            grad = lax.dot_general(v_peer, err[0, rows, :], NT, preferred_element_type=jnp.float32)
            grad += lax.dot_general(v_own, err[1, rows, :], NT, preferred_element_type=jnp.float32)
            u = users[:, rows]
            users[:, rows] = u - eta * (grad + lam * u)
        refresh_users(users[...])

    def step_items(t, q, c):
        k, slot = STEPS * t + q, q % 2
        cols = pl.ds(c * CHUNK, CHUNK)
        edge_slot = lax.rem(t, 2)
        if q < STEPS - 1:
            @pl.when(t > 0)
            def _():
                for p in range(PIECES):
                    item_copy(k - STEPS, q, c, p).wait_send()
        else:
            @pl.when(t > 1)
            def _():
                edge_own(t - 2, c).wait_send()
                for p in range(PIECES):
                    edge_peer(t - 2, c, p).wait_send()
        for p in range(PIECES):
            at = pl.ds(p * piece, piece)
            part_copy(k, slot, c, p).wait_recv()
            v = own[at, cols]
            v = v - eta * ((part[at, cols] + recv_p[k, c, at]) + lam * v)
            v_bf = v.astype(jnp.bfloat16)
            if q < STEPS - 1:
                own_next[q, c, at] = v_bf
                item_copy(k, q, c, p).start()
                own[at, cols] = v
                own_bf[(q + 1) % 2, at, cols] = v_bf
            else:
                edge_b[edge_slot, c, at] = v_bf

                @pl.when(t < n_sub_epochs - 1)
                def _():
                    edge_peer(t, c, p).start()
                edge_f[edge_slot, c, at] = v
        if q == STEPS - 1:
            @pl.when(t < n_sub_epochs - 1)
            def _():
                edge_own(t, c).start()

            @pl.when(t == n_sub_epochs - 1)
            def _():
                edge_last(t, c).start()
                edge_end(t, c).start()

    def sub_epoch(t, carry):
        @pl.when((t > 0) & (t < n_blk))
        def _():
            for copy in load(t, 0):
                copy.wait()
        for core, order in enumerate(ORDERS):
            @pl.when(lax.rem(blk, 2) == core)
            def _():
                for q in range(STEPS):
                    for op in order:
                        c = int(op[1:] or 0)
                        if op[0] == 'A':
                            send_part(t, q, c)
                        elif op[0] == 'D' and q > 0:
                            step_items(t, q - 1, c)
                        elif op[0] == 'B':
                            own_part(t, q)
                        elif op[0] == 'C':
                            step_items(t, q, c)
                        elif op[0] == 'M':
                            step_users(t, q)
                for op in order:
                    if op[0] == 'D':
                        step_items(t, STEPS - 1, int(op[1:]))
        return carry

    lax.fori_loop(0, n_sub_epochs, sub_epoch, 0)

    u_back = pltpu.make_async_copy(users, u_out, uv_sem.at[0])
    u_back.start()
    end = n_sub_epochs - 1
    last_k = STEPS * n_sub_epochs - 1
    for c in range(n_chunks):
        edge_end(end, c).wait_recv()
        edge_last(end, c).wait_recv()
    for c in range(n_chunks):
        for p in range(PIECES):
            part_copy(last_k - 1, 0, c, p).wait_send()
            part_copy(last_k, 1, c, p).wait_send()
            for q in range(STEPS - 1):
                item_copy(STEPS * end + q, q, c, p).wait_send()
        edge_own(end - 1, c).wait_send()
        for p in range(PIECES):
            edge_peer(end - 1, c, p).wait_send()
        edge_end(end, c).wait_send()
        edge_last(end, c).wait_send()
    u_back.wait()


def solution(mesh):
    n_blk = mesh.shape['blk']
    n_sub = mesh.shape['sub']
    row_spec = P(('rep', 'blk', 'sub'), None)
    item_spec = P(('rep', 'blk'), None)

    def local_run(ratings, mask, user_init, item_init):
        n_users = ratings.shape[0]
        n_items, rank = item_init.shape
        half = n_items // n_sub
        n_chunks = half // CHUNK
        n_sub_epochs = EPOCHS * n_blk
        n_steps = STEPS * n_sub_epochs
        wide = 128
        big_side = max(n_items, n_sub * n_users)
        eta = STEP_GAIN * math.sqrt(rank) / (math.sqrt(big_side) + math.sqrt(rank)) ** 2
        lam = DECAY / eta
        f32, bf16 = jnp.float32, jnp.bfloat16
        dma = pltpu.SemaphoreType.DMA
        chunk = (rank, CHUNK)
        any_space = pl.BlockSpec(memory_space=pl.ANY)
        in_hbm = functools.partial(pltpu.with_memory_space_constraint, memory_space=pltpu.HBM)
        users_t, items_t = pl.pallas_call(
            functools.partial(run, n_blk, eta, lam),
            out_shape=[jax.ShapeDtypeStruct((rank, n_users), f32), jax.ShapeDtypeStruct((rank, n_items), f32)],
            in_specs=[any_space] * 4,
            out_specs=[any_space] * 2,
            scratch_shapes=[
                pltpu.VMEM((n_blk, 2, n_users, half), f32),
                pltpu.VMEM((n_blk, 2, n_users, half), jnp.int32),
                pltpu.VMEM((2, n_users, half), bf16),
                pltpu.VMEM((rank, n_users), f32),
                pltpu.VMEM((n_users, wide), bf16),
                pltpu.VMEM((rank, n_users), bf16),
                pltpu.VMEM((rank, half), f32),
                pltpu.VMEM((2, rank, half), bf16),
                pltpu.VMEM((STEPS - 1, n_chunks) + chunk, bf16),
                pltpu.VMEM((rank, half), f32),
                pltpu.VMEM((2, n_chunks) + chunk, f32),
                pltpu.VMEM((n_steps, n_chunks) + chunk, f32),
                pltpu.VMEM((n_steps + 1, n_chunks) + chunk, bf16),
                pltpu.VMEM((n_sub_epochs, n_chunks) + chunk, f32),
                pltpu.VMEM((rank, n_items), f32),
                pltpu.VMEM((2, n_chunks) + chunk, f32),
                pltpu.VMEM((2, n_chunks) + chunk, bf16),
                dma((n_blk, 2, 2)),
                dma((n_chunks, 2)),
                dma((2,)),
                dma((2, n_chunks, PIECES)),
                dma((2, n_chunks, PIECES)),
                dma((STEPS - 1, n_chunks, PIECES)),
                dma((n_chunks, PIECES)),
                dma((2, n_chunks)),
                dma((n_sub_epochs, n_chunks)),
                dma((2, n_chunks, PIECES)),
                dma((n_sub_epochs, n_chunks, PIECES)),
                dma((n_chunks,)),
                dma((n_chunks,)),
            ],
            compiler_params=pltpu.CompilerParams(
                collective_id=0, has_side_effects=True, vmem_limit_bytes=52_000_000),
        )(ratings, mask, in_hbm(user_init.T), in_hbm(item_init.T))
        return users_t.T, items_t.T

    return jax.shard_map(local_run, mesh=mesh, in_specs=(row_spec, row_spec, row_spec, item_spec), out_specs=(row_spec, item_spec), check_vma=False)
```

```python
import functools
import math

import jax
import jax.numpy as jnp
from jax import lax
from jax.experimental import pallas as pl
from jax.experimental.pallas import tpu as pltpu
from jax.sharding import PartitionSpec as P

STEPS = 4
EPOCHS = 2
STEP_GAIN = 0.4
DECAY = 0.002
CHUNK = 128
ROWS = 256
PIECES = 2
ORDERS = (
    ('A0', 'A1', 'A2', 'A3', 'B', 'C0', 'M', 'C1', 'C2', 'C3'),
    ('A0', 'A1', 'D2', 'D3', 'B', 'C0', 'A2', 'C1', 'A3', 'M'),
)
MESH = pl.DeviceIdType.MESH
NT = (((1,), (1,)), ((), ()))


def run(n_blk, eta, lam, r_hbm, m_hbm, u_hbm, v_hbm, u_out, v_out,
        rate, known, err, users, users_bf, users_t, own, own_bf, own_next, part, send_p, recv_p,
        peer_v, in_v, v_start, edge_f, edge_b,
        load_sem, first_sem, uv_sem, p_send, p_recv, v_send, v_recv,
        ef_send, ef_recv, eb_send, eb_recv, el_send, el_recv):
    rank, n_users = users.shape
    half = own.shape[1]
    n_chunks = half // CHUNK
    n_sub_epochs = EPOCHS * n_blk
    pad = users_bf.shape[1] - rank
    me = lax.axis_index('sub')
    other = 1 - me
    blk = lax.axis_index('blk')
    down = lax.rem(blk + n_blk - 1, n_blk)
    up = lax.rem(blk + 1, n_blk)

    def load(t, role):
        owner = me if role else other
        col = pl.multiple_of(lax.rem(blk + t, n_blk) * (2 * half) + owner * half, half)
        return [
            pltpu.make_async_copy(src.at[:, pl.ds(col, half)], dst.at[t, role], load_sem.at[t, role, j])
            for j, (src, dst) in enumerate(((r_hbm, rate), (m_hbm, known)))
        ]

    def first_load(c):
        col = pl.multiple_of(blk * (2 * half) + other * half + c * CHUNK, CHUNK)
        return [
            pltpu.make_async_copy(src.at[:, pl.ds(col, CHUNK)], dst.at[0, 0, :, pl.ds(c * CHUNK, CHUNK)], first_sem.at[c, j])
            for j, (src, dst) in enumerate(((r_hbm, rate), (m_hbm, known)))
        ]

    def start_load(t):
        for role in range(2):
            for copy in load(t, role):
                copy.start()

    u_copy = pltpu.make_async_copy(u_hbm, users, uv_sem.at[0])
    v_copy = pltpu.make_async_copy(v_hbm, v_start, uv_sem.at[1])
    u_copy.start()
    v_copy.start()
    for c in range(n_chunks):
        for copy in first_load(c):
            copy.start()

    barrier = pltpu.get_barrier_semaphore()
    friends = [(blk, other), (down, me), (down, other), (up, me), (up, other)]
    for b, s in friends:
        pl.semaphore_signal(barrier, inc=1, device_id={'sub': s, 'blk': b}, device_id_type=MESH)

    def refresh_users(u):
        u_bf = u.astype(jnp.bfloat16)
        users_t[...] = u_bf
        wide = jnp.concatenate([u, jnp.zeros((pad, n_users), jnp.float32)], axis=0)
        users_bf[...] = wide.T.astype(jnp.bfloat16)

    u_copy.wait()
    refresh_users(users[...])
    v_copy.wait()

    def mine(c):
        return pl.ds(pl.multiple_of(me * half + c * CHUNK, CHUNK), CHUNK)

    for c in range(n_chunks):
        theirs = pl.ds(pl.multiple_of(other * half + c * CHUNK, CHUNK), CHUNK)
        in_v[0, c] = v_start[:, mine(c)]
        peer_v[0, c] = v_start[:, theirs].astype(jnp.bfloat16)
    pl.semaphore_wait(barrier, len(friends))

    def remote(src, dst, send, recv, s, b):
        return pltpu.make_async_remote_copy(
            src_ref=src, dst_ref=dst, send_sem=send, recv_sem=recv,
            device_id={'sub': s, 'blk': b}, device_id_type=MESH)

    piece = rank // PIECES

    def part_copy(k, slot, c, p):
        at = pl.ds(p * piece, piece)
        return remote(send_p.at[slot, c, at], recv_p.at[k, c, at], p_send.at[slot, c, p], p_recv.at[slot, c, p], other, blk)

    def item_copy(k, q, c, p):
        at = pl.ds(p * piece, piece)
        return remote(own_next.at[q, c, at], peer_v.at[k + 1, c, at], v_send.at[q, c, p], v_recv.at[c, p], other, blk)

    def edge_own(t, c):
        slot = lax.rem(t, 2)
        return remote(edge_f.at[slot, c], in_v.at[t + 1, c], ef_send.at[slot, c], ef_recv.at[t, c], me, down)

    def edge_peer(t, c):
        slot = lax.rem(t, 2)
        return remote(edge_b.at[slot, c], peer_v.at[STEPS * (t + 1), c], eb_send.at[slot, c], eb_recv.at[t, c], other, down)

    def edge_last(t, c):
        slot = lax.rem(t, 2)
        return remote(edge_f.at[slot, c], v_out.at[:, mine(c)], el_send.at[c], el_recv.at[c], other, down)

    def edge_end(t, c):
        slot = lax.rem(t, 2)
        return remote(edge_f.at[slot, c], v_out.at[:, mine(c)], ef_send.at[slot, c], ef_recv.at[t, c], me, down)

    def widen(v):
        return jnp.concatenate([v, jnp.zeros((pad, v.shape[1]), v.dtype)], axis=0)

    def errors(tm, role, cols, v_bf):
        v_wide = widen(v_bf)
        for r in range(0, n_users, ROWS):
            rows = pl.ds(r, ROWS)
            pred = jnp.dot(users_bf[rows, :], v_wide, preferred_element_type=jnp.float32)
            diff = jnp.where(known[tm, role, rows, cols] != 0, pred - rate[tm, role, rows, cols], 0.0)
            err[role, rows, cols] = diff.astype(jnp.bfloat16)

    def send_part(t, q, c):
        k, slot = STEPS * t + q, q % 2
        if q == 0:
            @pl.when(t == 0)
            def _():
                for copy in first_load(c):
                    copy.wait()
                if c == 1:
                    for copy in load(0, 1):
                        copy.start()

            @pl.when(t > 0)
            def _():
                edge_peer(t - 1, c).wait_recv()
        else:
            for p in range(PIECES):
                item_copy(k - 1, q - 1, c, p).wait_recv()
        cols = pl.ds(c * CHUNK, CHUNK)
        errors(lax.rem(t, n_blk), 0, cols, peer_v[k, c])
        total = jnp.dot(users_t[...], err[0, :, cols], preferred_element_type=jnp.float32)
        for p in range(PIECES):
            if q < 2:
                @pl.when(t > 0)
                def _():
                    part_copy(k - 2, slot, c, p).wait_send()
            else:
                part_copy(k - 2, slot, c, p).wait_send()
        send_p[slot, c] = total
        for p in range(PIECES):
            part_copy(k, slot, c, p).start()

    def own_part(t, q):
        if q == 0:
            @pl.when(t + 1 < n_blk)
            def _():
                start_load(t + 1)

            @pl.when(t < n_blk)
            def _():
                for copy in load(t, 1):
                    copy.wait()
            for c in range(n_chunks):
                @pl.when(t > 0)
                def _():
                    edge_own(t - 1, c).wait_recv()
                v = in_v[t, c]
                own[:, pl.ds(c * CHUNK, CHUNK)] = v
                own_bf[0, :, pl.ds(c * CHUNK, CHUNK)] = v.astype(jnp.bfloat16)
        for c in range(0, half, 256):
            cols = pl.ds(c, 256)
            errors(lax.rem(t, n_blk), 1, cols, own_bf[q % 2, :, cols])
            part[:, cols] = jnp.dot(users_t[...], err[1, :, cols], preferred_element_type=jnp.float32)

    def step_users(t, q):
        k = STEPS * t + q
        v_peer = jnp.concatenate([peer_v[k, c] for c in range(n_chunks)], axis=1)
        v_own = own_bf[q % 2]
        for r in range(0, n_users, ROWS):
            rows = pl.ds(r, ROWS)
            grad = lax.dot_general(v_peer, err[0, rows, :], NT, preferred_element_type=jnp.float32)
            grad += lax.dot_general(v_own, err[1, rows, :], NT, preferred_element_type=jnp.float32)
            u = users[:, rows]
            users[:, rows] = u - eta * (grad + lam * u)
        refresh_users(users[...])

    def step_items(t, q, c):
        k, slot = STEPS * t + q, q % 2
        cols = pl.ds(c * CHUNK, CHUNK)
        edge_slot = lax.rem(t, 2)
        if q < STEPS - 1:
            @pl.when(t > 0)
            def _():
                for p in range(PIECES):
                    item_copy(k - STEPS, q, c, p).wait_send()
        else:
            @pl.when(t > 1)
            def _():
                edge_own(t - 2, c).wait_send()
                edge_peer(t - 2, c).wait_send()
        for p in range(PIECES):
            at = pl.ds(p * piece, piece)
            part_copy(k, slot, c, p).wait_recv()
            v = own[at, cols]
            v = v - eta * ((part[at, cols] + recv_p[k, c, at]) + lam * v)
            v_bf = v.astype(jnp.bfloat16)
            if q < STEPS - 1:
                own_next[q, c, at] = v_bf
                item_copy(k, q, c, p).start()
                own[at, cols] = v
                own_bf[(q + 1) % 2, at, cols] = v_bf
            else:
                edge_f[edge_slot, c, at] = v
                edge_b[edge_slot, c, at] = v_bf
        if q == STEPS - 1:
            @pl.when(t < n_sub_epochs - 1)
            def _():
                edge_peer(t, c).start()
                edge_own(t, c).start()

            @pl.when(t == n_sub_epochs - 1)
            def _():
                edge_last(t, c).start()
                edge_end(t, c).start()

    def sub_epoch(t, carry):
        @pl.when((t > 0) & (t < n_blk))
        def _():
            for copy in load(t, 0):
                copy.wait()
        for core, order in enumerate(ORDERS):
            @pl.when(lax.rem(blk, 2) == core)
            def _():
                for q in range(STEPS):
                    for op in order:
                        c = int(op[1:] or 0)
                        if op[0] == 'A':
                            send_part(t, q, c)
                        elif op[0] == 'D' and q > 0:
                            step_items(t, q - 1, c)
                        elif op[0] == 'B':
                            own_part(t, q)
                        elif op[0] == 'C':
                            step_items(t, q, c)
                        elif op[0] == 'M':
                            step_users(t, q)
                for op in order:
                    if op[0] == 'D':
                        step_items(t, STEPS - 1, int(op[1:]))
        return carry

    lax.fori_loop(0, n_sub_epochs, sub_epoch, 0)

    u_back = pltpu.make_async_copy(users, u_out, uv_sem.at[0])
    u_back.start()
    end = n_sub_epochs - 1
    last_k = STEPS * n_sub_epochs - 1
    for c in range(n_chunks):
        edge_end(end, c).wait_recv()
        edge_last(end, c).wait_recv()
    for c in range(n_chunks):
        for p in range(PIECES):
            part_copy(last_k - 1, 0, c, p).wait_send()
            part_copy(last_k, 1, c, p).wait_send()
            for q in range(STEPS - 1):
                item_copy(STEPS * end + q, q, c, p).wait_send()
        edge_own(end - 1, c).wait_send()
        edge_peer(end - 1, c).wait_send()
        edge_end(end, c).wait_send()
        edge_last(end, c).wait_send()
    u_back.wait()


def solution(mesh):
    n_blk = mesh.shape['blk']
    n_sub = mesh.shape['sub']
    row_spec = P(('rep', 'blk', 'sub'), None)
    item_spec = P(('rep', 'blk'), None)

    def local_run(ratings, mask, user_init, item_init):
        n_users = ratings.shape[0]
        n_items, rank = item_init.shape
        half = n_items // n_sub
        n_chunks = half // CHUNK
        n_sub_epochs = EPOCHS * n_blk
        n_steps = STEPS * n_sub_epochs
        wide = 128
        big_side = max(n_items, n_sub * n_users)
        eta = STEP_GAIN * math.sqrt(rank) / (math.sqrt(big_side) + math.sqrt(rank)) ** 2
        lam = DECAY / eta
        f32, bf16 = jnp.float32, jnp.bfloat16
        dma = pltpu.SemaphoreType.DMA
        chunk = (rank, CHUNK)
        any_space = pl.BlockSpec(memory_space=pl.ANY)
        in_hbm = functools.partial(pltpu.with_memory_space_constraint, memory_space=pltpu.HBM)
        users_t, items_t = pl.pallas_call(
            functools.partial(run, n_blk, eta, lam),
            out_shape=[jax.ShapeDtypeStruct((rank, n_users), f32), jax.ShapeDtypeStruct((rank, n_items), f32)],
            in_specs=[any_space] * 4,
            out_specs=[any_space] * 2,
            scratch_shapes=[
                pltpu.VMEM((n_blk, 2, n_users, half), f32),
                pltpu.VMEM((n_blk, 2, n_users, half), jnp.int32),
                pltpu.VMEM((2, n_users, half), bf16),
                pltpu.VMEM((rank, n_users), f32),
                pltpu.VMEM((n_users, wide), bf16),
                pltpu.VMEM((rank, n_users), bf16),
                pltpu.VMEM((rank, half), f32),
                pltpu.VMEM((2, rank, half), bf16),
                pltpu.VMEM((STEPS - 1, n_chunks) + chunk, bf16),
                pltpu.VMEM((rank, half), f32),
                pltpu.VMEM((2, n_chunks) + chunk, f32),
                pltpu.VMEM((n_steps, n_chunks) + chunk, f32),
                pltpu.VMEM((n_steps + 1, n_chunks) + chunk, bf16),
                pltpu.VMEM((n_sub_epochs, n_chunks) + chunk, f32),
                pltpu.VMEM((rank, n_items), f32),
                pltpu.VMEM((2, n_chunks) + chunk, f32),
                pltpu.VMEM((2, n_chunks) + chunk, bf16),
                dma((n_blk, 2, 2)),
                dma((n_chunks, 2)),
                dma((2,)),
                dma((2, n_chunks, PIECES)),
                dma((2, n_chunks, PIECES)),
                dma((STEPS - 1, n_chunks, PIECES)),
                dma((n_chunks, PIECES)),
                dma((2, n_chunks)),
                dma((n_sub_epochs, n_chunks)),
                dma((2, n_chunks)),
                dma((n_sub_epochs, n_chunks)),
                dma((n_chunks,)),
                dma((n_chunks,)),
            ],
            compiler_params=pltpu.CompilerParams(
                collective_id=0, has_side_effects=True, vmem_limit_bytes=52_000_000),
        )(ratings, mask, in_hbm(user_init.T), in_hbm(item_init.T))
        return users_t.T, items_t.T

    return jax.shard_map(local_run, mesh=mesh, in_specs=(row_spec, row_spec, row_spec, item_spec), out_specs=(row_spec, item_spec), check_vma=False)
```

```python
import functools
import math

import jax
import jax.numpy as jnp
from jax import lax
from jax.experimental import pallas as pl
from jax.experimental.pallas import tpu as pltpu
from jax.sharding import PartitionSpec as P

STEPS = 4
EPOCHS = 2
STEP_GAIN = 0.4
DECAY = 0.002
CHUNK = 128
ROWS = 256
PIECES = 2
FIRST = ('A0', 'A1', 'A2', 'A3', 'B', 'C0', 'M', 'C1', 'C2', 'C3')
MIDDLE = ('A0', 'A1', 'D2', 'D3', 'B', 'C0', 'A2', 'C1', 'A3', 'M')
ORDERS = (
    (FIRST, FIRST, FIRST, FIRST),
    (
        ('A0', 'A1', 'B', 'C0', 'A2', 'C1', 'A3', 'M'),
        MIDDLE,
        MIDDLE,
        ('A0', 'A1', 'D2', 'D3', 'B', 'C0', 'C1', 'A2', 'A3', 'M', 'C2', 'C3'),
    ),
)
MESH = pl.DeviceIdType.MESH
NT = (((1,), (1,)), ((), ()))


def run(n_blk, eta, lam, r_hbm, m_hbm, u_hbm, v_hbm, u_out, v_out,
        rate, known, err, users, users_bf, users_t, own, own_bf, own_next, part, send_p, recv_p,
        peer_v, in_v, v_start, edge_f, edge_b,
        load_sem, uv_sem, p_send, p_recv, v_send, v_recv,
        ef_send, ef_recv, eb_send, eb_recv, el_send, el_recv):
    rank, n_users = users.shape
    half = own.shape[1]
    n_chunks = half // CHUNK
    n_sub_epochs = EPOCHS * n_blk
    pad = users_bf.shape[1] - rank
    me = lax.axis_index('sub')
    other = 1 - me
    blk = lax.axis_index('blk')
    down = lax.rem(blk + n_blk - 1, n_blk)
    up = lax.rem(blk + 1, n_blk)

    def load(t, role):
        owner = me if role else other
        col = pl.multiple_of(lax.rem(blk + t, n_blk) * (2 * half) + owner * half, half)
        return [
            pltpu.make_async_copy(src.at[:, pl.ds(col, half)], dst.at[t, role], load_sem.at[t, role, j])
            for j, (src, dst) in enumerate(((r_hbm, rate), (m_hbm, known)))
        ]

    def start_load(t):
        for role in range(2):
            for copy in load(t, role):
                copy.start()

    u_copy = pltpu.make_async_copy(u_hbm, users, uv_sem.at[0])
    v_copy = pltpu.make_async_copy(v_hbm, v_start, uv_sem.at[1])
    u_copy.start()
    v_copy.start()
    for copy in load(0, 0):
        copy.start()

    barrier = pltpu.get_barrier_semaphore()
    friends = [(blk, other), (down, me), (down, other), (up, me), (up, other)]
    for b, s in friends:
        pl.semaphore_signal(barrier, inc=1, device_id={'sub': s, 'blk': b}, device_id_type=MESH)

    def refresh_users(u):
        u_bf = u.astype(jnp.bfloat16)
        users_t[...] = u_bf
        wide = jnp.concatenate([u, jnp.zeros((pad, n_users), jnp.float32)], axis=0)
        users_bf[...] = wide.T.astype(jnp.bfloat16)

    u_copy.wait()
    refresh_users(users[...])
    v_copy.wait()

    def mine(c):
        return pl.ds(pl.multiple_of(me * half + c * CHUNK, CHUNK), CHUNK)

    for c in range(n_chunks):
        theirs = pl.ds(pl.multiple_of(other * half + c * CHUNK, CHUNK), CHUNK)
        in_v[0, c] = v_start[:, mine(c)]
        peer_v[0, c] = v_start[:, theirs].astype(jnp.bfloat16)
    for copy in load(0, 0):
        copy.wait()
    for copy in load(0, 1):
        copy.start()
    pl.semaphore_wait(barrier, len(friends))

    def remote(src, dst, send, recv, s, b):
        return pltpu.make_async_remote_copy(
            src_ref=src, dst_ref=dst, send_sem=send, recv_sem=recv,
            device_id={'sub': s, 'blk': b}, device_id_type=MESH)

    piece = rank // PIECES

    def part_copy(k, slot, c, p):
        at = pl.ds(p * piece, piece)
        return remote(send_p.at[slot, c, at], recv_p.at[k, c, at], p_send.at[slot, c, p], p_recv.at[slot, c, p], other, blk)

    def item_copy(k, q, c, p):
        at = pl.ds(p * piece, piece)
        return remote(own_next.at[q, c, at], peer_v.at[k + 1, c, at], v_send.at[q, c, p], v_recv.at[c, p], other, blk)

    def edge_own(t, c):
        slot = lax.rem(t, 2)
        return remote(edge_f.at[slot, c], in_v.at[t + 1, c], ef_send.at[slot, c], ef_recv.at[t, c], me, down)

    def edge_peer(t, c):
        slot = lax.rem(t, 2)
        return remote(edge_b.at[slot, c], peer_v.at[STEPS * (t + 1), c], eb_send.at[slot, c], eb_recv.at[t, c], other, down)

    def edge_last(t, c):
        slot = lax.rem(t, 2)
        return remote(edge_f.at[slot, c], v_out.at[:, mine(c)], el_send.at[c], el_recv.at[c], other, down)

    def edge_end(t, c):
        slot = lax.rem(t, 2)
        return remote(edge_f.at[slot, c], v_out.at[:, mine(c)], ef_send.at[slot, c], ef_recv.at[t, c], me, down)

    def widen(v):
        return jnp.concatenate([v, jnp.zeros((pad, v.shape[1]), v.dtype)], axis=0)

    def errors(tm, role, cols, v_bf):
        v_wide = widen(v_bf)
        for r in range(0, n_users, ROWS):
            rows = pl.ds(r, ROWS)
            pred = jnp.dot(users_bf[rows, :], v_wide, preferred_element_type=jnp.float32)
            diff = jnp.where(known[tm, role, rows, cols] != 0, pred - rate[tm, role, rows, cols], 0.0)
            err[role, rows, cols] = diff.astype(jnp.bfloat16)

    def send_part(t, q, c):
        k, slot = STEPS * t + q, q % 2
        if q == 0:
            @pl.when(t > 0)
            def _():
                edge_peer(t - 1, c).wait_recv()
        else:
            for p in range(PIECES):
                item_copy(k - 1, q - 1, c, p).wait_recv()
        cols = pl.ds(c * CHUNK, CHUNK)
        errors(lax.rem(t, n_blk), 0, cols, peer_v[k, c])
        total = jnp.dot(users_t[...], err[0, :, cols], preferred_element_type=jnp.float32)
        for p in range(PIECES):
            if q < 2:
                @pl.when(t > 0)
                def _():
                    part_copy(k - 2, slot, c, p).wait_send()
            else:
                part_copy(k - 2, slot, c, p).wait_send()
        send_p[slot, c] = total
        for p in range(PIECES):
            part_copy(k, slot, c, p).start()

    def own_part(t, q):
        if q == 0:
            @pl.when(t + 1 < n_blk)
            def _():
                start_load(t + 1)

            @pl.when(t < n_blk)
            def _():
                for copy in load(t, 1):
                    copy.wait()
            for c in range(n_chunks):
                @pl.when(t > 0)
                def _():
                    edge_own(t - 1, c).wait_recv()
                v = in_v[t, c]
                own[:, pl.ds(c * CHUNK, CHUNK)] = v
                own_bf[0, :, pl.ds(c * CHUNK, CHUNK)] = v.astype(jnp.bfloat16)
        for c in range(0, half, 256):
            cols = pl.ds(c, 256)
            errors(lax.rem(t, n_blk), 1, cols, own_bf[q % 2, :, cols])
            part[:, cols] = jnp.dot(users_t[...], err[1, :, cols], preferred_element_type=jnp.float32)

    def step_users(t, q):
        k = STEPS * t + q
        v_peer = jnp.concatenate([peer_v[k, c] for c in range(n_chunks)], axis=1)
        v_own = own_bf[q % 2]
        for r in range(0, n_users, ROWS):
            rows = pl.ds(r, ROWS)
            grad = lax.dot_general(v_peer, err[0, rows, :], NT, preferred_element_type=jnp.float32)
            grad += lax.dot_general(v_own, err[1, rows, :], NT, preferred_element_type=jnp.float32)
            u = users[:, rows]
            users[:, rows] = u - eta * (grad + lam * u)
        refresh_users(users[...])

    def step_items(t, q, c):
        k, slot = STEPS * t + q, q % 2
        cols = pl.ds(c * CHUNK, CHUNK)
        edge_slot = lax.rem(t, 2)
        if q < STEPS - 1:
            @pl.when(t > 0)
            def _():
                for p in range(PIECES):
                    item_copy(k - STEPS, q, c, p).wait_send()
        else:
            @pl.when(t > 1)
            def _():
                edge_own(t - 2, c).wait_send()
                edge_peer(t - 2, c).wait_send()
        for p in range(PIECES):
            at = pl.ds(p * piece, piece)
            part_copy(k, slot, c, p).wait_recv()
            v = own[at, cols]
            v = v - eta * ((part[at, cols] + recv_p[k, c, at]) + lam * v)
            v_bf = v.astype(jnp.bfloat16)
            if q < STEPS - 1:
                own_next[q, c, at] = v_bf
                item_copy(k, q, c, p).start()
                own[at, cols] = v
                own_bf[(q + 1) % 2, at, cols] = v_bf
            else:
                edge_f[edge_slot, c, at] = v
                edge_b[edge_slot, c, at] = v_bf
        if q == STEPS - 1:
            @pl.when(t < n_sub_epochs - 1)
            def _():
                edge_peer(t, c).start()
                edge_own(t, c).start()

            @pl.when(t == n_sub_epochs - 1)
            def _():
                edge_last(t, c).start()
                edge_end(t, c).start()

    def sub_epoch(t, carry):
        @pl.when((t > 0) & (t < n_blk))
        def _():
            for copy in load(t, 0):
                copy.wait()
        for core, orders in enumerate(ORDERS):
            @pl.when(lax.rem(blk, 2) == core)
            def _():
                for q in range(STEPS):
                    for op in orders[q]:
                        c = int(op[1:] or 0)
                        if op[0] == 'A':
                            send_part(t, q, c)
                        elif op[0] == 'B':
                            own_part(t, q)
                        elif op[0] == 'C':
                            step_items(t, q, c)
                        elif op[0] == 'D':
                            step_items(t, q - 1, c)
                        else:
                            step_users(t, q)
        return carry

    lax.fori_loop(0, n_sub_epochs, sub_epoch, 0)

    u_back = pltpu.make_async_copy(users, u_out, uv_sem.at[0])
    u_back.start()
    end = n_sub_epochs - 1
    last_k = STEPS * n_sub_epochs - 1
    for c in range(n_chunks):
        edge_end(end, c).wait_recv()
        edge_last(end, c).wait_recv()
    for c in range(n_chunks):
        for p in range(PIECES):
            part_copy(last_k - 1, 0, c, p).wait_send()
            part_copy(last_k, 1, c, p).wait_send()
            for q in range(STEPS - 1):
                item_copy(STEPS * end + q, q, c, p).wait_send()
        edge_own(end - 1, c).wait_send()
        edge_peer(end - 1, c).wait_send()
        edge_end(end, c).wait_send()
        edge_last(end, c).wait_send()
    u_back.wait()


def solution(mesh):
    n_blk = mesh.shape['blk']
    n_sub = mesh.shape['sub']
    row_spec = P(('rep', 'blk', 'sub'), None)
    item_spec = P(('rep', 'blk'), None)

    def local_run(ratings, mask, user_init, item_init):
        n_users = ratings.shape[0]
        n_items, rank = item_init.shape
        half = n_items // n_sub
        n_chunks = half // CHUNK
        n_sub_epochs = EPOCHS * n_blk
        n_steps = STEPS * n_sub_epochs
        wide = 128
        big_side = max(n_items, n_sub * n_users)
        eta = STEP_GAIN * math.sqrt(rank) / (math.sqrt(big_side) + math.sqrt(rank)) ** 2
        lam = DECAY / eta
        f32, bf16 = jnp.float32, jnp.bfloat16
        dma = pltpu.SemaphoreType.DMA
        chunk = (rank, CHUNK)
        any_space = pl.BlockSpec(memory_space=pl.ANY)
        in_hbm = functools.partial(pltpu.with_memory_space_constraint, memory_space=pltpu.HBM)
        users_t, items_t = pl.pallas_call(
            functools.partial(run, n_blk, eta, lam),
            out_shape=[jax.ShapeDtypeStruct((rank, n_users), f32), jax.ShapeDtypeStruct((rank, n_items), f32)],
            in_specs=[any_space] * 4,
            out_specs=[any_space] * 2,
            scratch_shapes=[
                pltpu.VMEM((n_blk, 2, n_users, half), f32),
                pltpu.VMEM((n_blk, 2, n_users, half), jnp.int32),
                pltpu.VMEM((2, n_users, half), bf16),
                pltpu.VMEM((rank, n_users), f32),
                pltpu.VMEM((n_users, wide), bf16),
                pltpu.VMEM((rank, n_users), bf16),
                pltpu.VMEM((rank, half), f32),
                pltpu.VMEM((2, rank, half), bf16),
                pltpu.VMEM((STEPS - 1, n_chunks) + chunk, bf16),
                pltpu.VMEM((rank, half), f32),
                pltpu.VMEM((2, n_chunks) + chunk, f32),
                pltpu.VMEM((n_steps, n_chunks) + chunk, f32),
                pltpu.VMEM((n_steps + 1, n_chunks) + chunk, bf16),
                pltpu.VMEM((n_sub_epochs, n_chunks) + chunk, f32),
                pltpu.VMEM((rank, n_items), f32),
                pltpu.VMEM((2, n_chunks) + chunk, f32),
                pltpu.VMEM((2, n_chunks) + chunk, bf16),
                dma((n_blk, 2, 2)),
                dma((2,)),
                dma((2, n_chunks, PIECES)),
                dma((2, n_chunks, PIECES)),
                dma((STEPS - 1, n_chunks, PIECES)),
                dma((n_chunks, PIECES)),
                dma((2, n_chunks)),
                dma((n_sub_epochs, n_chunks)),
                dma((2, n_chunks)),
                dma((n_sub_epochs, n_chunks)),
                dma((n_chunks,)),
                dma((n_chunks,)),
            ],
            compiler_params=pltpu.CompilerParams(
                collective_id=0, has_side_effects=True, vmem_limit_bytes=52_000_000),
        )(ratings, mask, in_hbm(user_init.T), in_hbm(item_init.T))
        return users_t.T, items_t.T

    return jax.shard_map(local_run, mesh=mesh, in_specs=(row_spec, row_spec, row_spec, item_spec), out_specs=(row_spec, item_spec), check_vma=False)
```
